16 devices in a mesh: tp: 2 (over z), dp: 2 (over y), pp: 4 (over x, core).
Axes of the slice: x: 2, y: 2, z: 2, core: 2. Of those that a mesh axis runs over, the one named last changes fastest.
Arguments:
- x_in: bfloat16 [6, 4, 256, 1536], P(None, 'dp', 'tp')
- g_out: bfloat16 [6, 4, 256, 1536], P(None, 'dp', 'tp')
- w_gate: bfloat16 [4, 1, 1536, 6144], P('pp', None, 'dp', 'tp')
- w_in: bfloat16 [4, 1, 1536, 6144], P('pp', None, 'dp', 'tp')
- w_out: bfloat16 [4, 1, 6144, 1536], P('pp', None, 'tp', 'dp')
Outputs:
- output 1: bfloat16 [6, 4, 256, 1536], P(None, 'dp', 'tp')
- output 2: float32 [4, 1, 1536, 6144], P('pp', None, 'dp', 'tp')
- output 3: float32 [4, 1, 1536, 6144], P('pp', None, 'dp', 'tp')
- output 4: float32 [4, 1, 6144, 1536], P('pp', None, 'tp', 'dp')
All inputs are finite; a program needn't handle non-finite values.
Results may differ from the reference program's by a relative error of at most 0.02.
Values are sent between devices in bfloat16 or wider.
A program may use at most 1 GiB of HBM per device.

```python
import jax
import jax.numpy as jnp
from jax import lax

STAGES = 4
LAYERS = 1
NUM_MICRO = 6
BATCH_ROWS = 4
SEQLEN = 256
HIDDEN = 1536
FFN_DIM = 6144
RMS_EPS = 1e-6


def setup_inputs(seed: int = 0) -> dict:
    rng_keys = jax.random.split(jax.random.key(seed), 5)
    act_shape = (NUM_MICRO, BATCH_ROWS, SEQLEN, HIDDEN)
    up_shape = (STAGES, LAYERS, HIDDEN, FFN_DIM)
    cot_scale = float(NUM_MICRO * BATCH_ROWS * SEQLEN) ** -0.25
    x_in = jax.random.normal(rng_keys[0], act_shape, jnp.float32).astype(jnp.bfloat16)
    g_out = (jax.random.normal(rng_keys[1], act_shape, jnp.float32) * cot_scale).astype(jnp.bfloat16)
    w_gate = (jax.random.normal(rng_keys[2], up_shape, jnp.float32) * HIDDEN ** -0.5).astype(jnp.bfloat16)
    w_in = (jax.random.normal(rng_keys[3], up_shape, jnp.float32) * HIDDEN ** -0.5).astype(jnp.bfloat16)
    w_out = (jax.random.normal(rng_keys[4], (STAGES, LAYERS, FFN_DIM, HIDDEN), jnp.float32) * FFN_DIM ** -0.5).astype(jnp.bfloat16)
    return {'x_in': x_in, 'g_out': g_out, 'w_gate': w_gate, 'w_in': w_in, 'w_out': w_out}


def rms_parts(h_tok):
    h_f32 = h_tok.astype(jnp.float32)
    inv_rms = lax.rsqrt(jnp.mean(h_f32 * h_f32, axis=-1, keepdims=True) + RMS_EPS)
    return h_f32, inv_rms, (h_f32 * inv_rms).astype(jnp.bfloat16)


def swiglu_parts(normed, w_gate_l, w_in_l):
    gate_pre = jnp.dot(normed, w_gate_l, preferred_element_type=jnp.float32)
    in_pre = jnp.dot(normed, w_in_l, preferred_element_type=jnp.float32)
    gate_sig = jax.nn.sigmoid(gate_pre)
    return gate_pre, in_pre, gate_sig, gate_pre * gate_sig


def layer_forward(h_tok, w_gate_l, w_in_l, w_out_l):
    normed = rms_parts(h_tok)[2]
    gate_pre, in_pre, gate_sig, gate_act = swiglu_parts(normed, w_gate_l, w_in_l)
    hidden = (gate_act * in_pre).astype(jnp.bfloat16)
    branch = jnp.dot(hidden, w_out_l, preferred_element_type=jnp.float32)
    return h_tok + branch.astype(jnp.bfloat16)


def layer_backward(h_tok, d_out, w_gate_l, w_in_l, w_out_l):
    h_f32, inv_rms, normed = rms_parts(h_tok)
    gate_pre, in_pre, gate_sig, gate_act = swiglu_parts(normed, w_gate_l, w_in_l)
    hidden = (gate_act * in_pre).astype(jnp.bfloat16)
    grad_out = jnp.dot(hidden.T, d_out, preferred_element_type=jnp.float32)
    d_hidden = jnp.dot(d_out, w_out_l.T, preferred_element_type=jnp.float32).astype(jnp.bfloat16).astype(jnp.float32)
    d_gate = (d_hidden * in_pre * (gate_sig * (1.0 + gate_pre * (1.0 - gate_sig)))).astype(jnp.bfloat16)
    d_up = (d_hidden * gate_act).astype(jnp.bfloat16)
    grad_gate = jnp.dot(normed.T, d_gate, preferred_element_type=jnp.float32)
    grad_in = jnp.dot(normed.T, d_up, preferred_element_type=jnp.float32)
    d_norm = jnp.dot(d_gate, w_gate_l.T, preferred_element_type=jnp.float32) + jnp.dot(d_up, w_in_l.T, preferred_element_type=jnp.float32)
    unit_rms = h_f32 * inv_rms
    d_h = inv_rms * (d_norm - unit_rms * jnp.mean(d_norm * unit_rms, axis=-1, keepdims=True))
    return (d_out.astype(jnp.float32) + d_h).astype(jnp.bfloat16), grad_gate, grad_in, grad_out


def reference(x_in, g_out, w_gate, w_in, w_out):
    n_layers = STAGES * LAYERS
    tokens = BATCH_ROWS * SEQLEN
    w_gate_all = w_gate.reshape(n_layers, HIDDEN, FFN_DIM)
    w_in_all = w_in.reshape(n_layers, HIDDEN, FFN_DIM)
    w_out_all = w_out.reshape(n_layers, FFN_DIM, HIDDEN)

    def micro_step(grads, micro_pair):
        x_mb, g_mb = micro_pair

        def fwd_body(h_tok, weights):
            return layer_forward(h_tok, weights[0], weights[1], weights[2]), h_tok

        fwd_last, saved = lax.scan(fwd_body, x_mb.reshape(tokens, HIDDEN), (w_gate_all, w_in_all, w_out_all))

        def bwd_body(d_h, layer_in):
            d_prev, grad_gate, grad_in, grad_out = layer_backward(layer_in[0], d_h, layer_in[1], layer_in[2], layer_in[3])
            return d_prev, (grad_gate, grad_in, grad_out)

        d_first, layer_grads = lax.scan(bwd_body, g_mb.reshape(tokens, HIDDEN), (saved, w_gate_all, w_in_all, w_out_all), reverse=True)
        new_grads = tuple(acc + part for acc, part in zip(grads, layer_grads))
        return new_grads, d_first.reshape(BATCH_ROWS, SEQLEN, HIDDEN)

    start = (jnp.zeros((n_layers, HIDDEN, FFN_DIM), jnp.float32), jnp.zeros((n_layers, HIDDEN, FFN_DIM), jnp.float32), jnp.zeros((n_layers, FFN_DIM, HIDDEN), jnp.float32))
    grads, dx_in = lax.scan(micro_step, start, (x_in, g_out))
    return (dx_in, grads[0].reshape(STAGES, LAYERS, HIDDEN, FFN_DIM), grads[1].reshape(STAGES, LAYERS, HIDDEN, FFN_DIM), grads[2].reshape(STAGES, LAYERS, FFN_DIM, HIDDEN))
```

```python
import jax
import jax.numpy as jnp
from jax import lax
from jax.sharding import Mesh, PartitionSpec as P

RMS_EPS = 1e-6
CONTRACT_ROWS = (((0,), (0,)), ((), ()))
CONTRACT_COLS = (((1,), (1,)), ((), ()))
ALL_AXES = ('tp', 'dp', 'x', 'core')
LAG = 2


def device(z, y, x, core):
    return ((z * 2 + y) * 2 + x) * 2 + core


def pairs(move):
    found = []
    for z in range(2):
        for y in range(2):
            for x in range(2):
                for core in range(2):
                    target = move(z, y, x, core)
                    if target is not None:
                        found.append((device(z, y, x, core), device(*target)))
    return found


ACROSS_Z = pairs(lambda z, y, x, c: (1 - z, y, x, c))
ACROSS_CORE = pairs(lambda z, y, x, c: (z, y, x, 1 - c))
HOME_SWAP = pairs(lambda z, y, x, c: (z, 1 - y, x, 1 - c) if c != y else None)
X_TO_FIRST = pairs(lambda z, y, x, c: (z, 0, 0, 1) if (y, x, c) == (1, 0, 1) else None)
G_TO_LAST = pairs(lambda z, y, x, c: (z, 1, 1, 0) if (y, x, c) == (0, 1, 0) else None)
STAGE_UP = pairs(lambda z, y, x, c: (z, (2 * x + y + 1) % 2, (2 * x + y + 1) // 2, c) if 2 * x + y < 3 else None)
STAGE_DOWN = pairs(lambda z, y, x, c: (z, (2 * x + y - 1) % 2, (2 * x + y - 1) // 2, c) if 2 * x + y > 0 else None)
DX_Y = pairs(lambda z, y, x, c: (z, 1, 0, 1) if (y, x, c) == (0, 0, 1) else None)
DX_X = pairs(lambda z, y, x, c: (z, y, 1, c) if x == 0 and c == y else None)
DX_CORE = pairs(lambda z, y, x, c: (z, y, x, 1 - c) if c == y else None)


def send(value, table):
    return lax.ppermute(value, ALL_AXES, table)


def rms_parts(h_tok):
    h_f32 = h_tok.astype(jnp.float32)
    inv_rms = lax.rsqrt(jnp.mean(h_f32 * h_f32, axis=-1, keepdims=True) + RMS_EPS)
    return h_f32, inv_rms, (h_f32 * inv_rms).astype(jnp.bfloat16)


def swiglu_parts(normed_all, w_gate_l, w_in_l):
    gate_pre = jnp.dot(normed_all, w_gate_l, preferred_element_type=jnp.float32)
    in_pre = jnp.dot(normed_all, w_in_l, preferred_element_type=jnp.float32)
    gate_sig = jax.nn.sigmoid(gate_pre)
    return gate_pre, in_pre, gate_sig, gate_pre * gate_sig


def put(buffer, value, slot, valid):
    if valid is not None:
        value = jnp.where(valid, value, lax.dynamic_index_in_dim(buffer, slot, 0, keepdims=False))
    return lax.dynamic_update_index_in_dim(buffer, value, slot, 0)


def solution(mesh):
    fine = Mesh(mesh.devices.reshape(2, 2, 2, 2), ALL_AXES)
    act_spec = P(None, 'dp', 'tp', None)
    up_spec = P(('x', 'core'), None, 'dp', 'tp')
    down_spec = P(('x', 'core'), None, 'tp', 'dp')
    n_stages = 4

    def train_step(x_in, g_out, w_gate, w_in, w_out):
        y = lax.axis_index('dp')
        x = lax.axis_index('x')
        core = lax.axis_index('core')
        stage = 2 * x + y
        at_home = core == y
        n_micro, rows_seq, rows, width = x_in.shape
        n_chunks = n_micro * rows_seq
        n_steps = n_chunks + LAG * (n_stages - 1)

        def stage_weight(w_home, axis):
            block = jnp.where(at_home, w_home, send(w_home, HOME_SWAP))
            other = send(block, ACROSS_CORE)
            return jnp.where(core == 0, jnp.concatenate([block, other], axis), jnp.concatenate([other, block], axis))

        w_gate_s = stage_weight(w_gate[0, 0], 0)
        w_in_s = stage_weight(w_in[0, 0], 0)
        w_out_s = stage_weight(w_out[0, 0], 1)

        def chunks_of(array, table, take):
            found = []
            for micro in range(n_micro):
                mine = jnp.where(take, send(array[micro], table), array[micro])
                found.extend(mine[seq] for seq in range(rows_seq))
            return found

        x_chunks = chunks_of(x_in, X_TO_FIRST, core == 1)
        g_chunks = chunks_of(g_out, G_TO_LAST, core == 0)

        saved_h = jnp.zeros((n_chunks, rows, width), jnp.bfloat16)
        saved_n = jnp.zeros((n_chunks, 2 * rows, width), jnp.bfloat16)
        received = [jnp.zeros((rows, width), jnp.bfloat16)] * LAG
        for step in range(n_steps):
            chunk = step - LAG * stage
            slot = jnp.clip(chunk, 0, n_chunks - 1)
            valid = chunk < n_chunks if step >= n_chunks else None
            h_tok = jnp.where(stage == 0, x_chunks[min(step, n_chunks - 1)], received[step])
            normed = rms_parts(h_tok)[2]
            normed_all = jnp.concatenate([normed, send(normed, ACROSS_Z)], 0)
            saved_h = put(saved_h, h_tok, slot, valid)
            saved_n = put(saved_n, normed_all, slot, valid)
            gate_pre, in_pre, gate_sig, gate_act = swiglu_parts(normed_all, w_gate_s, w_in_s)
            hidden = (gate_act * in_pre).astype(jnp.bfloat16)
            if step + LAG < n_steps:
                branch = jnp.dot(hidden, w_out_s, preferred_element_type=jnp.float32)
                branch = branch[:rows] + send(branch[rows:], ACROSS_Z)
                received.append(send(h_tok + branch.astype(jnp.bfloat16), STAGE_UP))

        hid = w_gate_s.shape[1]
        saved_e = jnp.zeros((n_chunks, 2 * rows, width), jnp.bfloat16)
        saved_u = jnp.zeros((n_chunks, 2 * rows, hid), jnp.bfloat16)
        saved_da = jnp.zeros((n_chunks, 2 * rows, hid), jnp.bfloat16)
        saved_db = jnp.zeros((n_chunks, 2 * rows, hid), jnp.bfloat16)
        received = [jnp.zeros((rows, width), jnp.bfloat16)] * LAG
        dx_chunks = []
        for step in range(n_steps):
            chunk = step - LAG * (n_stages - 1 - stage)
            slot = jnp.clip(chunk, 0, n_chunks - 1)
            valid = chunk < n_chunks if step >= n_chunks else None
            d_out = jnp.where(stage == n_stages - 1, g_chunks[min(step, n_chunks - 1)], received[step])
            d_all = jnp.concatenate([d_out, send(d_out, ACROSS_Z)], 0)
            h_tok = lax.dynamic_index_in_dim(saved_h, slot, 0, keepdims=False)
            normed_all = lax.dynamic_index_in_dim(saved_n, slot, 0, keepdims=False)
            h_f32, inv_rms, _ = rms_parts(h_tok)
            gate_pre, in_pre, gate_sig, gate_act = swiglu_parts(normed_all, w_gate_s, w_in_s)
            hidden = (gate_act * in_pre).astype(jnp.bfloat16)
            d_hidden = lax.dot_general(d_all, w_out_s, CONTRACT_COLS, preferred_element_type=jnp.float32).astype(jnp.bfloat16).astype(jnp.float32)
            d_gate = (d_hidden * in_pre * (gate_sig * (1.0 + gate_pre * (1.0 - gate_sig)))).astype(jnp.bfloat16)
            d_up = (d_hidden * gate_act).astype(jnp.bfloat16)
            saved_e = put(saved_e, d_all, slot, valid)
            saved_u = put(saved_u, hidden, slot, valid)
            saved_da = put(saved_da, d_gate, slot, valid)
            saved_db = put(saved_db, d_up, slot, valid)
            d_norm = lax.dot_general(d_gate, w_gate_s, CONTRACT_COLS, preferred_element_type=jnp.float32) + lax.dot_general(d_up, w_in_s, CONTRACT_COLS, preferred_element_type=jnp.float32)
            d_norm = d_norm[:rows] + send(d_norm[rows:], ACROSS_Z)
            unit_rms = h_f32 * inv_rms
            d_h = inv_rms * (d_norm - unit_rms * jnp.mean(d_norm * unit_rms, axis=-1, keepdims=True))
            d_prev = (d_out.astype(jnp.float32) + d_h).astype(jnp.bfloat16)
            if step + LAG < n_steps:
                received.append(send(d_prev, STAGE_DOWN))
            if step >= n_steps - n_chunks:
                dx_chunks.append(d_prev)

        dx_micros = []
        for micro in range(n_micro):
            dx = jnp.stack(dx_chunks[micro * rows_seq:(micro + 1) * rows_seq])
            dx = jnp.where((x == 0) & (y == 1) & (core == 1), send(dx, DX_Y), dx)
            dx = jnp.where((x == 1) & at_home, send(dx, DX_X), dx)
            dx_micros.append(jnp.where(at_home, dx, send(dx, DX_CORE)))
        dx_in = jnp.stack(dx_micros)

        half = width // 2
        tokens = n_chunks * 2 * rows
        n_flat = saved_n.reshape(tokens, width)
        e_flat = saved_e.reshape(tokens, width)

        def half_of(flat, which):
            return lax.dynamic_slice_in_dim(flat, which * half, half, 1)

        def grad_home(product, flat):
            theirs = send(product(half_of(flat, 1 - core)), ACROSS_CORE)
            total = product(half_of(flat, core)) + theirs
            return jnp.where(at_home, total, send(total, HOME_SWAP))[None, None]

        def against(cot):
            flat = cot.reshape(tokens, hid)
            return lambda part: lax.dot_general(part, flat, CONTRACT_ROWS, preferred_element_type=jnp.float32)

        u_flat = saved_u.reshape(tokens, hid)
        dw_out = grad_home(lambda part: lax.dot_general(u_flat, part, CONTRACT_ROWS, preferred_element_type=jnp.float32), e_flat)
        dw_gate = grad_home(against(saved_da), n_flat)
        dw_in = grad_home(against(saved_db), n_flat)
        return dx_in, dw_gate, dw_in, dw_out

    return jax.shard_map(train_step, mesh=fine, in_specs=(act_spec, act_spec, up_spec, up_spec, down_spec), out_specs=(act_spec, up_spec, up_spec, down_spec), check_vma=False)
```

```python
import jax
import jax.numpy as jnp
from jax import lax
from jax.experimental import pallas as pl
from jax.experimental.pallas import tpu as pltpu
from jax.sharding import Mesh, PartitionSpec as P

RMS_EPS = 1e-6
CONTRACT_ROWS = (((0,), (0,)), ((), ()))
CONTRACT_COLS = (((1,), (1,)), ((), ()))
ALL_AXES = ('tp', 'dp', 'x', 'core')
COLS = 512
ROWS = 64
DEPTH = 6
VMEM_BYTES = 60 * 1024 * 1024


def device(z, y, x, core):
    return ((z * 2 + y) * 2 + x) * 2 + core


def pairs(move):
    found = []
    for z in range(2):
        for y in range(2):
            for x in range(2):
                for core in range(2):
                    target = move(z, y, x, core)
                    if target is not None:
                        found.append((device(z, y, x, core), device(*target)))
    return found


ACROSS_Z = pairs(lambda z, y, x, c: (1 - z, y, x, c))
ACROSS_CORE = pairs(lambda z, y, x, c: (z, y, x, 1 - c))
HOME_SWAP = pairs(lambda z, y, x, c: (z, 1 - y, x, 1 - c) if c != y else (z, y, x, c))
X_TO_FIRST = pairs(lambda z, y, x, c: (z, 0, 0, 1) if (y, x, c) == (1, 0, 1) else None)
G_TO_LAST = pairs(lambda z, y, x, c: (z, 1, 1, 0) if (y, x, c) == (0, 1, 0) else None)
DX_Y = pairs(lambda z, y, x, c: (z, 1, 0, 1) if (y, x, c) == (0, 0, 1) else None)
DX_X = pairs(lambda z, y, x, c: (z, y, 1, c) if x == 0 and c == y else None)
DX_CORE = pairs(lambda z, y, x, c: (z, y, x, 1 - c) if c == y else None)


def send(value, table):
    return lax.ppermute(value, ALL_AXES, table)


def rms_parts(h_tok):
    h_f32 = h_tok.astype(jnp.float32)
    inv_rms = lax.rsqrt(jnp.mean(h_f32 * h_f32, axis=-1, keepdims=True) + RMS_EPS)
    return h_f32, inv_rms, (h_f32 * inv_rms).astype(jnp.bfloat16)


def swiglu_parts(normed_all, w_gate_l, w_in_l):
    gate_pre = jnp.dot(normed_all, w_gate_l, preferred_element_type=jnp.float32)
    in_pre = jnp.dot(normed_all, w_in_l, preferred_element_type=jnp.float32)
    gate_sig = jax.nn.sigmoid(gate_pre)
    return gate_pre, in_pre, gate_sig, gate_pre * gate_sig


def stage_place():
    z, y, x, core = (lax.axis_index(name) for name in ALL_AXES)
    after = {'dp': 1 - y, 'x': x + y}
    before = {'dp': 1 - y, 'x': x + y - 1}
    return 2 * x + y, core, {'tp': 1 - z}, after, before


def remote(source, target, send_sem, recv_sem, place):
    return pltpu.make_async_remote_copy(src_ref=source, dst_ref=target, send_sem=send_sem, recv_sem=recv_sem, device_id=place, device_id_type=pl.DeviceIdType.MESH)


def weight_loads(core, blocks, w_gate, w_in, w_out, sems):
    half = w_gate.shape[0] // 2
    loads = []
    for k, which in enumerate((core, 1 - core)):
        part = pl.ds(pl.multiple_of(which * half, half), half)
        for j, (block, target) in enumerate(zip(blocks[3 * k:3 * k + 3], (w_gate.at[part], w_in.at[part], w_out.at[:, part]))):
            loads.append(pltpu.make_async_copy(block, target, sems.at[3 * k + j]))
    return loads


def forward_kernel(x_ref, *refs):
    blocks = refs[:6]
    saved_h, saved_n = refs[6:8]
    (w_gate, w_in, w_out, h_buf, n_own, n_peer, acc, keep, give, got, h_out,
     w_sem, load_sem, h_send, h_recv, n_send, n_recv, g_send, g_recv, save_h, save_own, save_peer, free) = refs[8:]
    n = x_ref.shape[0]
    rows = x_ref.shape[1]
    hid = w_gate.shape[1]
    stage, core, peer, after, before = stage_place()
    loads = weight_loads(core, blocks, w_gate, w_in, w_out, w_sem)
    for load in loads:
        load.start()

    def x_load(c):
        return pltpu.make_async_copy(x_ref.at[c], h_buf.at[lax.rem(c, DEPTH)], load_sem.at[lax.rem(c, 2)])

    def h_copy(c):
        return remote(h_out.at[lax.rem(c, 2)], h_buf.at[lax.rem(c, DEPTH)], h_send.at[lax.rem(c, 2)], h_recv.at[lax.rem(c, DEPTH)], after)

    def n_copy(c):
        s = lax.rem(c, 3)
        return remote(n_own.at[s], n_peer.at[s], n_send.at[s], n_recv.at[s], peer)

    def give_copy(c):
        s = lax.rem(c, 3)
        return remote(give.at[s], got.at[s], g_send.at[s], g_recv.at[s], peer)

    def keep_h(c):
        s = lax.rem(c, DEPTH)
        return pltpu.make_async_copy(h_buf.at[s], saved_h.at[c], save_h.at[s])

    def keep_own(c):
        s = lax.rem(c, 3)
        return pltpu.make_async_copy(n_own.at[s], saved_n.at[c, pl.ds(0, rows)], save_own.at[s])

    def keep_peer(c):
        s = lax.rem(c, 3)
        return pltpu.make_async_copy(n_peer.at[s], saved_n.at[c, pl.ds(rows, rows)], save_peer.at[s])

    @pl.when(stage == 0)
    def _():
        x_load(0).start()

    def body(i, carry):
        @pl.when(i < n)
        def _():
            @pl.when(stage == 0)
            def _():
                x_load(i).wait()

                @pl.when(i + 1 < n)
                def _():
                    x_load(i + 1).start()

            @pl.when(stage > 0)
            def _():
                h_copy(i).wait_recv()

            keep_h(i).start()

            @pl.when(i >= 3)
            def _():
                n_copy(i - 3).wait_send()
                keep_own(i - 3).wait()

            n_own[lax.rem(i, 3)] = rms_parts(h_buf[lax.rem(i, DEPTH)])[2]
            n_copy(i).start()
            keep_own(i).start()

        @pl.when(i == 1)
        def _():
            for load in loads:
                load.wait()

        @pl.when((i >= 1) & (i <= n))
        def _():
            c = i - 1
            s = lax.rem(c, 3)
            n_copy(c).wait_recv()
            keep_peer(c).start()
            both = jnp.concatenate([n_own[s], n_peer[s]], 0)
            for j in range(hid // COLS):
                part = pl.ds(j * COLS, COLS)
                gate_pre, in_pre, gate_sig, gate_act = swiglu_parts(both, w_gate[:, part], w_in[:, part])
                branch = jnp.dot((gate_act * in_pre).astype(jnp.bfloat16), w_out[part, :], preferred_element_type=jnp.float32)
                acc[...] = branch if j == 0 else acc[...] + branch
            keep[s] = acc[:rows]
            give[s] = acc[rows:]
            keep_peer(c).wait()
            give_copy(c).start()

        @pl.when(i >= 2)
        def _():
            c = i - 2
            s = lax.rem(c, 3)
            give_copy(c).wait_recv()
            give_copy(c).wait_send()
            keep_h(c).wait()

            @pl.when(stage < 3)
            def _():
                @pl.when(c >= 2)
                def _():
                    h_copy(c - 2).wait_send()

                h_out[lax.rem(c, 2)] = h_buf[lax.rem(c, DEPTH)] + (keep[s] + got[s]).astype(jnp.bfloat16)

                @pl.when(c >= DEPTH)
                def _():
                    pl.semaphore_wait(free, 1)

                h_copy(c).start()

            @pl.when((stage > 0) & (c < n - DEPTH))
            def _():
                pl.semaphore_signal(free, inc=1, device_id=before, device_id_type=pl.DeviceIdType.MESH)

        return carry

    lax.fori_loop(0, n + 2, body, 0)
    for c in range(n - 3, n):
        n_copy(c).wait_send()
        keep_own(c).wait()

    @pl.when(stage < 3)
    def _():
        for c in range(n - 2, n):
            h_copy(c).wait_send()


def backward_kernel(g_ref, saved_h, saved_n, *refs):
    blocks = refs[:6]
    dx_ref, saved_e, saved_u, saved_da, saved_db = refs[6:11]
    (w_gate, w_in, w_out, e_buf, e_peer, n_buf, h_buf, acc, keep, give, got, e_out, u_out, da_out, db_out,
     w_sem, load_sem, n_sem, h_sem, s_send, s_recv, e_send, e_recv, g_send, g_recv, save_own, save_peer, save_u, save_da, save_db, dx_sem, free) = refs[11:]
    n = g_ref.shape[0]
    rows = g_ref.shape[1]
    hid = w_gate.shape[1]
    stage, core, peer, after, before = stage_place()
    loads = weight_loads(core, blocks, w_gate, w_in, w_out, w_sem)
    for load in loads:
        load.start()

    def g_load(c):
        return pltpu.make_async_copy(g_ref.at[c], e_buf.at[lax.rem(c, DEPTH)], load_sem.at[lax.rem(c, 2)])

    def n_load(c):
        s = lax.rem(c, 3)
        return pltpu.make_async_copy(saved_n.at[c], n_buf.at[s], n_sem.at[s])

    def h_load(c):
        s = lax.rem(c, 3)
        return pltpu.make_async_copy(saved_h.at[c], h_buf.at[s], h_sem.at[s])

    def stage_copy(c):
        return remote(e_out.at[lax.rem(c, 2)], e_buf.at[lax.rem(c, DEPTH)], s_send.at[lax.rem(c, 2)], s_recv.at[lax.rem(c, DEPTH)], before)

    def e_copy(c):
        s = lax.rem(c, 3)
        return remote(e_buf.at[lax.rem(c, DEPTH)], e_peer.at[s], e_send.at[s], e_recv.at[s], peer)

    def give_copy(c):
        s = lax.rem(c, 3)
        return remote(give.at[s], got.at[s], g_send.at[s], g_recv.at[s], peer)

    def keep_own(c):
        return pltpu.make_async_copy(e_buf.at[lax.rem(c, DEPTH)], saved_e.at[c, pl.ds(0, rows)], save_own.at[lax.rem(c, 3)])

    def keep_peer(c):
        s = lax.rem(c, 3)
        return pltpu.make_async_copy(e_peer.at[s], saved_e.at[c, pl.ds(rows, rows)], save_peer.at[s])

    def keep_wide(c):
        s = lax.rem(c, 2)
        return [pltpu.make_async_copy(source.at[s], target.at[c], sem.at[s])
                for source, target, sem in ((u_out, saved_u, save_u), (da_out, saved_da, save_da), (db_out, saved_db, save_db))]

    def keep_dx(c):
        s = lax.rem(c, 2)
        return pltpu.make_async_copy(e_out.at[s], dx_ref.at[c], dx_sem.at[s])

    @pl.when(stage == 3)
    def _():
        g_load(0).start()

    def body(i, carry):
        @pl.when(i < n)
        def _():
            n_load(i).start()
            h_load(i).start()

            @pl.when(stage == 3)
            def _():
                g_load(i).wait()

                @pl.when(i + 1 < n)
                def _():
                    g_load(i + 1).start()

            @pl.when(stage < 3)
            def _():
                stage_copy(i).wait_recv()

            e_copy(i).start()
            keep_own(i).start()

        @pl.when(i == 1)
        def _():
            for load in loads:
                load.wait()

        @pl.when((i >= 1) & (i <= n))
        def _():
            c = i - 1
            s = lax.rem(c, 3)
            w = lax.rem(c, 2)
            n_load(c).wait()
            e_copy(c).wait_recv()
            keep_peer(c).start()

            @pl.when(c >= 2)
            def _():
                for copy in keep_wide(c - 2):
                    copy.wait()

            normed = n_buf[s]
            both = jnp.concatenate([e_buf[lax.rem(c, DEPTH)], e_peer[s]], 0)
            for j in range(hid // COLS):
                part = pl.ds(j * COLS, COLS)
                gate_pre, in_pre, gate_sig, gate_act = swiglu_parts(normed, w_gate[:, part], w_in[:, part])
                d_hidden = lax.dot_general(both, w_out[part, :], CONTRACT_COLS, preferred_element_type=jnp.float32).astype(jnp.bfloat16).astype(jnp.float32)
                u_out[w, :, part] = (gate_act * in_pre).astype(jnp.bfloat16)
                d_gate = (d_hidden * in_pre * (gate_sig * (1.0 + gate_pre * (1.0 - gate_sig)))).astype(jnp.bfloat16)
                d_up = (d_hidden * gate_act).astype(jnp.bfloat16)
                da_out[w, :, part] = d_gate
                db_out[w, :, part] = d_up
                d_norm = lax.dot_general(d_gate, w_gate[:, part], CONTRACT_COLS, preferred_element_type=jnp.float32) + lax.dot_general(d_up, w_in[:, part], CONTRACT_COLS, preferred_element_type=jnp.float32)
                acc[...] = d_norm if j == 0 else acc[...] + d_norm
            for copy in keep_wide(c):
                copy.start()
            keep[s] = acc[:rows]
            give[s] = acc[rows:]
            keep_peer(c).wait()
            give_copy(c).start()

        @pl.when(i >= 2)
        def _():
            c = i - 2
            s = lax.rem(c, 3)
            w = lax.rem(c, 2)
            h_load(c).wait()
            give_copy(c).wait_recv()
            give_copy(c).wait_send()
            e_copy(c).wait_send()
            keep_own(c).wait()

            @pl.when(c >= 2)
            def _():
                @pl.when(stage > 0)
                def _():
                    stage_copy(c - 2).wait_send()

                @pl.when(stage == 0)
                def _():
                    keep_dx(c - 2).wait()

            d_norm = keep[s] + got[s]
            h_f32, inv_rms, _ = rms_parts(h_buf[s])
            unit_rms = h_f32 * inv_rms
            d_h = inv_rms * (d_norm - unit_rms * jnp.mean(d_norm * unit_rms, axis=-1, keepdims=True))
            e_out[w] = (e_buf[lax.rem(c, DEPTH)].astype(jnp.float32) + d_h).astype(jnp.bfloat16)

            @pl.when(stage > 0)
            def _():
                @pl.when(c >= DEPTH)
                def _():
                    pl.semaphore_wait(free, 1)

                stage_copy(c).start()

            @pl.when(stage == 0)
            def _():
                keep_dx(c).start()

            @pl.when((stage < 3) & (c < n - DEPTH))
            def _():
                pl.semaphore_signal(free, inc=1, device_id=after, device_id_type=pl.DeviceIdType.MESH)

        return carry

    lax.fori_loop(0, n + 2, body, 0)
    for c in range(n - 2, n):
        for copy in keep_wide(c):
            copy.wait()

        @pl.when(stage > 0)
        def _():
            stage_copy(c).wait_send()

        @pl.when(stage == 0)
        def _():
            keep_dx(c).wait()


def common_scratch(width, hid, rows):
    return [pltpu.VMEM((width, hid), jnp.bfloat16), pltpu.VMEM((width, hid), jnp.bfloat16), pltpu.VMEM((hid, width), jnp.bfloat16),
            pltpu.VMEM((DEPTH, rows, width), jnp.bfloat16)]


def partial_scratch(width, rows):
    return [pltpu.VMEM((2 * rows, width), jnp.float32)] + [pltpu.VMEM((3, rows, width), jnp.float32)] * 3 + [pltpu.VMEM((2, rows, width), jnp.bfloat16)]


def dma(*sizes):
    return [pltpu.SemaphoreType.DMA((size,)) for size in sizes]


def forward_phase(x_chunks, blocks):
    n, rows, width = x_chunks.shape
    hid = blocks[0].shape[1]
    anywhere = pl.BlockSpec(memory_space=pl.ANY)
    return pl.pallas_call(
        forward_kernel,
        in_specs=[anywhere] * 7,
        out_specs=[anywhere] * 2,
        out_shape=[jax.ShapeDtypeStruct((n, rows, width), jnp.bfloat16), jax.ShapeDtypeStruct((n, 2 * rows, width), jnp.bfloat16)],
        scratch_shapes=common_scratch(width, hid, rows) + [pltpu.VMEM((3, rows, width), jnp.bfloat16)] * 2 + partial_scratch(width, rows)
        + dma(6, 2, 2, DEPTH, 3, 3, 3, 3, DEPTH, 3, 3) + [pltpu.SemaphoreType.REGULAR],
        cost_estimate=pl.CostEstimate(flops=12 * n * rows * width * hid, bytes_accessed=6 * width * hid, transcendentals=0),
        compiler_params=pltpu.CompilerParams(has_side_effects=True, vmem_limit_bytes=VMEM_BYTES),
        name="forward_phase",
    )(x_chunks, *blocks)


def backward_phase(g_chunks, saved_h, saved_n, blocks):
    n, rows, width = g_chunks.shape
    hid = blocks[0].shape[1]
    anywhere = pl.BlockSpec(memory_space=pl.ANY)
    wide = jax.ShapeDtypeStruct((n, 2 * rows, hid), jnp.bfloat16)
    return pl.pallas_call(
        backward_kernel,
        in_specs=[anywhere] * 9,
        out_specs=[anywhere] * 5,
        out_shape=[jax.ShapeDtypeStruct((n, rows, width), jnp.bfloat16), jax.ShapeDtypeStruct((n, 2 * rows, width), jnp.bfloat16), wide, wide, wide],
        scratch_shapes=common_scratch(width, hid, rows)
        + [pltpu.VMEM((3, rows, width), jnp.bfloat16), pltpu.VMEM((3, 2 * rows, width), jnp.bfloat16), pltpu.VMEM((3, rows, width), jnp.bfloat16)]
        + partial_scratch(width, rows) + [pltpu.VMEM((2, 2 * rows, hid), jnp.bfloat16)] * 3
        + dma(6, 2, 3, 3, 2, DEPTH, 3, 3, 3, 3, 3, 3, 2, 2, 2, 2) + [pltpu.SemaphoreType.REGULAR],
        cost_estimate=pl.CostEstimate(flops=20 * n * rows * width * hid, bytes_accessed=6 * width * hid, transcendentals=0),
        compiler_params=pltpu.CompilerParams(has_side_effects=True, vmem_limit_bytes=VMEM_BYTES),
        name="backward_phase",
    )(g_chunks, saved_h, saved_n, *blocks)


def solution(mesh):
    fine = Mesh(mesh.devices.reshape(2, 2, 2, 2), ALL_AXES)
    act_spec = P(None, 'dp', 'tp', None)
    up_spec = P(('x', 'core'), None, 'dp', 'tp')
    down_spec = P(('x', 'core'), None, 'tp', 'dp')

    def train_step(x_in, g_out, w_gate, w_in, w_out):
        y = lax.axis_index('dp')
        x = lax.axis_index('x')
        core = lax.axis_index('core')
        at_home = core == y
        width = x_in.shape[3]
        x_in_chunks = x_in.reshape(-1, ROWS, width)
        g_in_chunks = g_out.reshape(-1, ROWS, width)
        n_chunks = x_in_chunks.shape[0]

        own = [send(w[0, 0], HOME_SWAP) for w in (w_gate, w_in, w_out)]
        blocks = own + [send(block, ACROSS_CORE) for block in own]
        x_chunks = jnp.where(core == 1, send(x_in_chunks, X_TO_FIRST), x_in_chunks)
        g_chunks = jnp.where(core == 0, send(g_in_chunks, G_TO_LAST), g_in_chunks)
        saved_h, saved_n = forward_phase(x_chunks, blocks)
        dx, saved_e, saved_u, saved_da, saved_db = backward_phase(g_chunks, saved_h, saved_n, blocks)

        dx = jnp.where((x == 0) & (y == 1) & (core == 1), send(dx, DX_Y), dx)
        dx = jnp.where((x == 1) & at_home, send(dx, DX_X), dx)
        dx_in = jnp.where(at_home, dx, send(dx, DX_CORE))

        half = width // 2
        tokens = n_chunks * 2 * ROWS

        def flat(array):
            return array.reshape(tokens, array.shape[-1])

        def half_of(array, which):
            return lax.dynamic_slice_in_dim(array, which * half, half, 1)

        def product(left, right):
            return lax.dot_general(left, right, CONTRACT_ROWS, preferred_element_type=jnp.float32)

        n_flat, e_flat, u_flat, da_flat, db_flat = flat(saved_n), flat(saved_e), flat(saved_u), flat(saved_da), flat(saved_db)
        out_theirs = send(product(u_flat, half_of(e_flat, 1 - core)), ACROSS_CORE)
        gate_theirs = send(product(half_of(n_flat, 1 - core), da_flat), ACROSS_CORE)
        out_total = product(u_flat, half_of(e_flat, core)) + out_theirs
        out_total, db_flat, dx_in = lax.optimization_barrier((out_total, db_flat, dx_in))
        dw_out = send(out_total, HOME_SWAP)[None, None]
        gate_total = product(half_of(n_flat, core), da_flat) + gate_theirs
        dw_gate = send(gate_total, HOME_SWAP)[None, None]
        in_theirs = send(product(half_of(n_flat, 1 - core), db_flat), ACROSS_CORE)
        dw_in = send(product(half_of(n_flat, core), db_flat) + in_theirs, HOME_SWAP)[None, None]
        return dx_in.reshape(x_in.shape), dw_gate, dw_in, dw_out

    return jax.shard_map(train_step, mesh=fine, in_specs=(act_spec, act_spec, up_spec, up_spec, down_spec), out_specs=(act_spec, up_spec, up_spec, down_spec), check_vma=False)
```

```python
import jax
import jax.numpy as jnp
from jax import lax
from jax.experimental import pallas as pl
from jax.experimental.pallas import tpu as pltpu
from jax.sharding import Mesh, PartitionSpec as P

RMS_EPS = 1e-6
CONTRACT_ROWS = (((0,), (0,)), ((), ()))
CONTRACT_COLS = (((1,), (1,)), ((), ()))
ALL_AXES = ('tp', 'dp', 'x', 'core')
COLS = 512
ROWS = 64
ROW_BLOCK = 256
DEPTH = 6
VMEM_BYTES = 60 * 1024 * 1024


def device(z, y, x, core):
    return ((z * 2 + y) * 2 + x) * 2 + core


def pairs(move):
    found = []
    for z in range(2):
        for y in range(2):
            for x in range(2):
                for core in range(2):
                    target = move(z, y, x, core)
                    if target is not None:
                        found.append((device(z, y, x, core), device(*target)))
    return found


ACROSS_Z = pairs(lambda z, y, x, c: (1 - z, y, x, c))
ACROSS_CORE = pairs(lambda z, y, x, c: (z, y, x, 1 - c))
HOME_SWAP = pairs(lambda z, y, x, c: (z, 1 - y, x, 1 - c) if c != y else (z, y, x, c))


def send(value, table):
    return lax.ppermute(value, ALL_AXES, table)


def rms_parts(h_tok):
    h_f32 = h_tok.astype(jnp.float32)
    inv_rms = lax.rsqrt(jnp.mean(h_f32 * h_f32, axis=-1, keepdims=True) + RMS_EPS)
    return h_f32, inv_rms, (h_f32 * inv_rms).astype(jnp.bfloat16)


def swiglu_parts(normed_all, w_gate_l, w_in_l):
    gate_pre = jnp.dot(normed_all, w_gate_l, preferred_element_type=jnp.float32)
    in_pre = jnp.dot(normed_all, w_in_l, preferred_element_type=jnp.float32)
    gate_sig = jax.nn.sigmoid(gate_pre)
    return gate_pre, in_pre, gate_sig, gate_pre * gate_sig


def stage_place():
    z, y, x, core = (lax.axis_index(name) for name in ALL_AXES)
    after = {'dp': 1 - y, 'x': x + y}
    before = {'dp': 1 - y, 'x': x + y - 1}
    return 2 * x + y, core, {'tp': 1 - z}, after, before


def remote(source, target, send_sem, recv_sem, place):
    return pltpu.make_async_remote_copy(src_ref=source, dst_ref=target, send_sem=send_sem, recv_sem=recv_sem, device_id=place, device_id_type=pl.DeviceIdType.MESH)


def weight_loads(core, blocks, w_gate, w_in, w_out, sems):
    half = w_gate.shape[0] // 2
    loads = []
    for k, which in enumerate((core, 1 - core)):
        part = pl.ds(pl.multiple_of(which * half, half), half)
        for j, (block, target) in enumerate(zip(blocks[3 * k:3 * k + 3], (w_gate.at[part], w_in.at[part], w_out.at[:, part]))):
            loads.append(pltpu.make_async_copy(block, target, sems.at[3 * k + j]))
    return loads


def forward_kernel(x_ref, *refs):
    blocks = refs[:6]
    saved_h, saved_n, x_land = refs[6:9]
    (w_gate, w_in, w_out, h_buf, n_own, n_peer, acc, keep, give, got, h_out,
     w_sem, load_sem, h_send, h_recv, n_send, n_recv, g_send, g_recv, save_h, save_own, save_peer, far_send, far_recv, free) = refs[9:]
    n = x_ref.shape[0]
    rows = x_ref.shape[1]
    hid = w_gate.shape[1]
    stage, core, peer, after, before = stage_place()
    loads = weight_loads(core, blocks, w_gate, w_in, w_out, w_sem)
    for load in loads:
        load.start()

    def x_load(c, source):
        return pltpu.make_async_copy(source.at[c], h_buf.at[lax.rem(c, DEPTH)], load_sem.at[lax.rem(c, 2)])

    def far_copy(c):
        return remote(x_ref.at[c], x_land.at[c], far_send.at[c], far_recv.at[c], {'dp': 0})

    def start_load(c):
        @pl.when(core == 0)
        def _():
            x_load(c, x_ref).start()

        @pl.when(core == 1)
        def _():
            far_copy(c).wait_recv()
            x_load(c, x_land).start()

    @pl.when((stage == 1) & (core == 1))
    def _():
        @pl.loop(0, n)
        def _(c):
            far_copy(c).start()

    def h_copy(c):
        return remote(h_out.at[lax.rem(c, 2)], h_buf.at[lax.rem(c, DEPTH)], h_send.at[lax.rem(c, 2)], h_recv.at[lax.rem(c, DEPTH)], after)

    def n_copy(c):
        s = lax.rem(c, 3)
        return remote(n_own.at[s], n_peer.at[s], n_send.at[s], n_recv.at[s], peer)

    def give_copy(c):
        s = lax.rem(c, 3)
        return remote(give.at[s], got.at[s], g_send.at[s], g_recv.at[s], peer)

    def keep_h(c):
        s = lax.rem(c, DEPTH)
        return pltpu.make_async_copy(h_buf.at[s], saved_h.at[c], save_h.at[s])

    def keep_own(c):
        s = lax.rem(c, 3)
        return pltpu.make_async_copy(n_own.at[s], saved_n.at[c, pl.ds(0, rows)], save_own.at[s])

    def keep_peer(c):
        s = lax.rem(c, 3)
        return pltpu.make_async_copy(n_peer.at[s], saved_n.at[c, pl.ds(rows, rows)], save_peer.at[s])

    @pl.when(stage == 0)
    def _():
        start_load(0)

    def body(i, carry):
        @pl.when(i < n)
        def _():
            @pl.when(stage == 0)
            def _():
                x_load(i, x_ref).wait()

                @pl.when(i + 1 < n)
                def _():
                    start_load(i + 1)

            @pl.when(stage > 0)
            def _():
                h_copy(i).wait_recv()

            keep_h(i).start()

            @pl.when(i >= 3)
            def _():
                n_copy(i - 3).wait_send()
                keep_own(i - 3).wait()

            n_own[lax.rem(i, 3)] = rms_parts(h_buf[lax.rem(i, DEPTH)])[2]
            n_copy(i).start()
            keep_own(i).start()

        @pl.when(i == 1)
        def _():
            for load in loads:
                load.wait()

        @pl.when((i >= 1) & (i <= n))
        def _():
            c = i - 1
            s = lax.rem(c, 3)
            n_copy(c).wait_recv()
            keep_peer(c).start()
            both = jnp.concatenate([n_own[s], n_peer[s]], 0)
            for j in range(hid // COLS):
                part = pl.ds(j * COLS, COLS)
                gate_pre, in_pre, gate_sig, gate_act = swiglu_parts(both, w_gate[:, part], w_in[:, part])
                branch = jnp.dot((gate_act * in_pre).astype(jnp.bfloat16), w_out[part, :], preferred_element_type=jnp.float32)
                acc[...] = branch if j == 0 else acc[...] + branch
            keep[s] = acc[:rows]
            give[s] = acc[rows:]
            keep_peer(c).wait()
            give_copy(c).start()

        @pl.when(i >= 2)
        def _():
            c = i - 2
            s = lax.rem(c, 3)
            give_copy(c).wait_recv()
            give_copy(c).wait_send()
            keep_h(c).wait()

            @pl.when(stage < 3)
            def _():
                @pl.when(c >= 2)
                def _():
                    h_copy(c - 2).wait_send()

                h_out[lax.rem(c, 2)] = h_buf[lax.rem(c, DEPTH)] + (keep[s] + got[s]).astype(jnp.bfloat16)

                @pl.when(c >= DEPTH)
                def _():
                    pl.semaphore_wait(free, 1)

                h_copy(c).start()

            @pl.when((stage > 0) & (c < n - DEPTH))
            def _():
                pl.semaphore_signal(free, inc=1, device_id=before, device_id_type=pl.DeviceIdType.MESH)

        return carry

    lax.fori_loop(0, n + 2, body, 0)
    for c in range(n - 3, n):
        n_copy(c).wait_send()
        keep_own(c).wait()

    @pl.when((stage == 1) & (core == 1))
    def _():
        @pl.loop(0, n)
        def _(c):
            far_copy(c).wait_send()

    @pl.when(stage < 3)
    def _():
        for c in range(n - 2, n):
            h_copy(c).wait_send()


def backward_kernel(g_ref, saved_h, saved_n, *refs):
    blocks = refs[:6]
    dx_ref, saved_e, saved_u, saved_da, saved_db, g_land = refs[6:12]
    (w_gate, w_in, w_out, e_buf, e_peer, n_buf, h_buf, acc, keep, give, got, e_out, u_out, da_out, db_out,
     w_sem, load_sem, n_sem, h_sem, s_send, s_recv, e_send, e_recv, g_send, g_recv, save_own, save_peer, save_u, save_da, save_db, dx_sem, dx_send, dx_recv, far_send, far_recv, free) = refs[12:]
    n = g_ref.shape[0]
    rows = g_ref.shape[1]
    hid = w_gate.shape[1]
    stage, core, peer, after, before = stage_place()
    loads = weight_loads(core, blocks, w_gate, w_in, w_out, w_sem)
    for load in loads:
        load.start()

    def g_load(c, source):
        return pltpu.make_async_copy(source.at[c], e_buf.at[lax.rem(c, DEPTH)], load_sem.at[lax.rem(c, 2)])

    def far_copy(c):
        return remote(g_ref.at[c], g_land.at[c], far_send.at[c], far_recv.at[c], {'dp': 1})

    def start_load(c):
        @pl.when(core == 1)
        def _():
            g_load(c, g_ref).start()

        @pl.when(core == 0)
        def _():
            far_copy(c).wait_recv()
            g_load(c, g_land).start()

    @pl.when((stage == 2) & (core == 0))
    def _():
        @pl.loop(0, n)
        def _(c):
            far_copy(c).start()

    def n_load(c):
        s = lax.rem(c, 3)
        return pltpu.make_async_copy(saved_n.at[c], n_buf.at[s], n_sem.at[s])

    def h_load(c):
        s = lax.rem(c, 3)
        return pltpu.make_async_copy(saved_h.at[c], h_buf.at[s], h_sem.at[s])

    def stage_copy(c):
        return remote(e_out.at[lax.rem(c, 2)], e_buf.at[lax.rem(c, DEPTH)], s_send.at[lax.rem(c, 2)], s_recv.at[lax.rem(c, DEPTH)], before)

    def e_copy(c):
        s = lax.rem(c, 3)
        return remote(e_buf.at[lax.rem(c, DEPTH)], e_peer.at[s], e_send.at[s], e_recv.at[s], peer)

    def give_copy(c):
        s = lax.rem(c, 3)
        return remote(give.at[s], got.at[s], g_send.at[s], g_recv.at[s], peer)

    def keep_own(c):
        return pltpu.make_async_copy(e_buf.at[lax.rem(c, DEPTH)], saved_e.at[c, pl.ds(0, rows)], save_own.at[lax.rem(c, 3)])

    def keep_peer(c):
        s = lax.rem(c, 3)
        return pltpu.make_async_copy(e_peer.at[s], saved_e.at[c, pl.ds(rows, rows)], save_peer.at[s])

    def keep_wide(c):
        s = lax.rem(c, 2)
        return [pltpu.make_async_copy(source.at[s], target.at[c], sem.at[s])
                for source, target, sem in ((u_out, saved_u, save_u), (da_out, saved_da, save_da), (db_out, saved_db, save_db))]

    def keep_dx(c):
        s = lax.rem(c, 2)
        return pltpu.make_async_copy(e_out.at[s], dx_ref.at[c], dx_sem.at[s])

    def dx_copy(c, k):
        s = lax.rem(c, 2)
        return remote(e_out.at[s], dx_ref.at[c], dx_send.at[s, k], dx_recv.at[0], {'dp': core, 'x': k // 2, 'core': k % 2})

    def dx_start(c):
        @pl.when(core == 0)
        def _():
            keep_dx(c).start()

        @pl.when(core == 1)
        def _():
            dx_copy(c, 0).start()

        for k in range(1, 4):
            dx_copy(c, k).start()

    def dx_done(c):
        @pl.when(core == 0)
        def _():
            keep_dx(c).wait()

        @pl.when(core == 1)
        def _():
            dx_copy(c, 0).wait_send()

        for k in range(1, 4):
            dx_copy(c, k).wait_send()

    @pl.when(stage == 3)
    def _():
        start_load(0)

    def body(i, carry):
        @pl.when(i < n)
        def _():
            n_load(i).start()
            h_load(i).start()

            @pl.when(stage == 3)
            def _():
                g_load(i, g_ref).wait()

                @pl.when(i + 1 < n)
                def _():
                    start_load(i + 1)

            @pl.when(stage < 3)
            def _():
                stage_copy(i).wait_recv()

            e_copy(i).start()
            keep_own(i).start()

        @pl.when(i == 1)
        def _():
            for load in loads:
                load.wait()

        @pl.when((i >= 1) & (i <= n))
        def _():
            c = i - 1
            s = lax.rem(c, 3)
            w = lax.rem(c, 2)
            n_load(c).wait()
            e_copy(c).wait_recv()
            keep_peer(c).start()

            @pl.when(c >= 2)
            def _():
                for copy in keep_wide(c - 2):
                    copy.wait()

            normed = n_buf[s]
            both = jnp.concatenate([e_buf[lax.rem(c, DEPTH)], e_peer[s]], 0)
            for j in range(hid // COLS):
                part = pl.ds(j * COLS, COLS)
                gate_pre, in_pre, gate_sig, gate_act = swiglu_parts(normed, w_gate[:, part], w_in[:, part])
                d_hidden = lax.dot_general(both, w_out[part, :], CONTRACT_COLS, preferred_element_type=jnp.float32).astype(jnp.bfloat16).astype(jnp.float32)
                u_out[w, :, part] = (gate_act * in_pre).astype(jnp.bfloat16)
                d_gate = (d_hidden * in_pre * (gate_sig * (1.0 + gate_pre * (1.0 - gate_sig)))).astype(jnp.bfloat16)
                d_up = (d_hidden * gate_act).astype(jnp.bfloat16)
                da_out[w, :, part] = d_gate
                db_out[w, :, part] = d_up
                d_norm = lax.dot_general(d_gate, w_gate[:, part], CONTRACT_COLS, preferred_element_type=jnp.float32) + lax.dot_general(d_up, w_in[:, part], CONTRACT_COLS, preferred_element_type=jnp.float32)
                acc[...] = d_norm if j == 0 else acc[...] + d_norm
            for copy in keep_wide(c):
                copy.start()
            keep[s] = acc[:rows]
            give[s] = acc[rows:]
            keep_peer(c).wait()
            give_copy(c).start()

        @pl.when(i >= 2)
        def _():
            c = i - 2
            s = lax.rem(c, 3)
            w = lax.rem(c, 2)
            h_load(c).wait()
            give_copy(c).wait_recv()
            give_copy(c).wait_send()
            e_copy(c).wait_send()
            keep_own(c).wait()

            @pl.when(c >= 2)
            def _():
                @pl.when(stage > 0)
                def _():
                    stage_copy(c - 2).wait_send()

                @pl.when(stage == 0)
                def _():
                    dx_done(c - 2)

            d_norm = keep[s] + got[s]
            h_f32, inv_rms, _ = rms_parts(h_buf[s])
            unit_rms = h_f32 * inv_rms
            d_h = inv_rms * (d_norm - unit_rms * jnp.mean(d_norm * unit_rms, axis=-1, keepdims=True))
            e_out[w] = (e_buf[lax.rem(c, DEPTH)].astype(jnp.float32) + d_h).astype(jnp.bfloat16)

            @pl.when(stage > 0)
            def _():
                @pl.when(c >= DEPTH)
                def _():
                    pl.semaphore_wait(free, 1)

                stage_copy(c).start()

            @pl.when(stage == 0)
            def _():
                dx_start(c)

            @pl.when((stage < 3) & (c < n - DEPTH))
            def _():
                pl.semaphore_signal(free, inc=1, device_id=after, device_id_type=pl.DeviceIdType.MESH)

        return carry

    lax.fori_loop(0, n + 2, body, 0)
    for c in range(n - 2, n):
        for copy in keep_wide(c):
            copy.wait()

        @pl.when(stage > 0)
        def _():
            stage_copy(c).wait_send()

        @pl.when(stage == 0)
        def _():
            dx_done(c)

    @pl.when((stage > 0) | (core > 0))
    def _():
        remote(dx_ref, dx_ref, dx_send.at[0, 0], dx_recv.at[0], peer).wait_recv()

    @pl.when((stage == 2) & (core == 0))
    def _():
        @pl.loop(0, n)
        def _(c):
            far_copy(c).wait_send()


def common_scratch(width, hid, rows):
    return [pltpu.VMEM((width, hid), jnp.bfloat16), pltpu.VMEM((width, hid), jnp.bfloat16), pltpu.VMEM((hid, width), jnp.bfloat16),
            pltpu.VMEM((DEPTH, rows, width), jnp.bfloat16)]


def partial_scratch(width, rows):
    return [pltpu.VMEM((2 * rows, width), jnp.float32)] + [pltpu.VMEM((3, rows, width), jnp.float32)] * 3 + [pltpu.VMEM((2, rows, width), jnp.bfloat16)]


def dma(*sizes):
    return [pltpu.SemaphoreType.DMA((size,)) for size in sizes]


def forward_phase(x_chunks, blocks):
    n, rows, width = x_chunks.shape
    hid = blocks[0].shape[1]
    anywhere = pl.BlockSpec(memory_space=pl.ANY)
    return pl.pallas_call(
        forward_kernel,
        in_specs=[anywhere] * 7,
        out_specs=[anywhere] * 3,
        out_shape=[jax.ShapeDtypeStruct((n, rows, width), jnp.bfloat16), jax.ShapeDtypeStruct((n, 2 * rows, width), jnp.bfloat16), jax.ShapeDtypeStruct((n, rows, width), jnp.bfloat16)],
        scratch_shapes=common_scratch(width, hid, rows) + [pltpu.VMEM((3, rows, width), jnp.bfloat16)] * 2 + partial_scratch(width, rows)
        + dma(6, 2, 2, DEPTH, 3, 3, 3, 3, DEPTH, 3, 3, n, n) + [pltpu.SemaphoreType.REGULAR],
        cost_estimate=pl.CostEstimate(flops=12 * n * rows * width * hid, bytes_accessed=6 * width * hid, transcendentals=0),
        compiler_params=pltpu.CompilerParams(has_side_effects=True, vmem_limit_bytes=VMEM_BYTES),
        name="forward_phase",
    )(x_chunks, *blocks)


def backward_phase(g_chunks, saved_h, saved_n, blocks):
    n, rows, width = g_chunks.shape
    hid = blocks[0].shape[1]
    anywhere = pl.BlockSpec(memory_space=pl.ANY)
    wide = jax.ShapeDtypeStruct((n, 2 * rows, hid), jnp.bfloat16)
    return pl.pallas_call(
        backward_kernel,
        in_specs=[anywhere] * 9,
        out_specs=[anywhere] * 6,
        out_shape=[jax.ShapeDtypeStruct((n, rows, width), jnp.bfloat16), jax.ShapeDtypeStruct((n, 2 * rows, width), jnp.bfloat16), wide, wide, wide, jax.ShapeDtypeStruct((n, rows, width), jnp.bfloat16)],
        scratch_shapes=common_scratch(width, hid, rows)
        + [pltpu.VMEM((3, rows, width), jnp.bfloat16), pltpu.VMEM((3, 2 * rows, width), jnp.bfloat16), pltpu.VMEM((3, rows, width), jnp.bfloat16)]
        + partial_scratch(width, rows) + [pltpu.VMEM((2, 2 * rows, hid), jnp.bfloat16)] * 3
        + dma(6, 2, 3, 3, 2, DEPTH, 3, 3, 3, 3, 3, 3, 2, 2, 2, 2) + [pltpu.SemaphoreType.DMA((2, 4))] + dma(1, n, n) + [pltpu.SemaphoreType.REGULAR],
        cost_estimate=pl.CostEstimate(flops=20 * n * rows * width * hid, bytes_accessed=6 * width * hid, transcendentals=0),
        compiler_params=pltpu.CompilerParams(has_side_effects=True, vmem_limit_bytes=VMEM_BYTES),
        name="backward_phase",
    )(g_chunks, saved_h, saved_n, *blocks)


def gradient_kernel(n_ref, e_ref, da_ref, db_ref, u_ref, dw_gate, dw_in, dw_out,
                    raw, flipped, tile, mine, give, got, total, total_t,
                    raw_sem, tile_sem, p_send, p_recv, keep_sem, keep_t_sem, far_send, far_t_send, far_recv):
    z, y, x, core = (lax.axis_index(name) for name in ALL_AXES)
    tokens, width = n_ref.shape
    hid = da_ref.shape[1]
    half = width // 2
    tiles = hid // COLS
    steps = tokens // COLS
    home = core == y
    swap = {'dp': 1 - y, 'core': 1 - core}
    sources = (da_ref, db_ref, u_ref)
    targets = (dw_gate, dw_in, dw_out)

    def cols(j):
        return pl.ds(pl.multiple_of(j * COLS, COLS), COLS)

    def raw_load(source, k):
        return pltpu.make_async_copy(source.at[cols(k)], raw.at[lax.rem(k, 2)], raw_sem.at[lax.rem(k, 2)])

    def tile_load(a, j):
        s = lax.rem(a * tiles + j, 2)
        return pltpu.make_async_copy(sources[a].at[:, cols(j)], tile.at[s], tile_sem.at[s])

    def part_copy(t):
        s = lax.rem(t, 2)
        return remote(give.at[s], got.at[s], p_send.at[s], p_recv.at[s], {'core': 1 - core})

    def place(a, j):
        return (total_t if a == 2 else total).at[lax.rem(j, 3)], (targets[a].at[cols(j)] if a == 2 else targets[a].at[:, cols(j)])

    def home_copy(a, j):
        source, target = place(a, j)
        return pltpu.make_async_copy(source, target, (keep_t_sem if a == 2 else keep_sem).at[lax.rem(j, 3)])

    def far_copy(a, j):
        source, target = place(a, j)
        return remote(source, target, (far_t_send if a == 2 else far_send).at[lax.rem(j, 3)], far_recv.at[a], swap)

    def shipped(a, j):
        @pl.when(home)
        def _():
            home_copy(a, j).wait()

        @pl.when(jnp.logical_not(home))
        def _():
            far_copy(a, j).wait_send()

    def flip(source):
        raw_load(source, 0).start()

        @pl.loop(0, steps)
        def _(k):
            raw_load(source, k).wait()

            @pl.when(k + 1 < steps)
            def _():
                raw_load(source, k + 1).start()

            flipped[:, cols(k)] = raw[lax.rem(k, 2)].T

    tile_load(0, 0).start()
    for a in range(3):
        if a != 1:
            flip(n_ref if a == 0 else e_ref)

        @pl.loop(0, tiles)
        def _(j, a=a):
            t = a * tiles + j
            s = lax.rem(t, 2)
            tile_load(a, j).wait()

            @pl.when(j + 1 < tiles)
            def _():
                tile_load(a, j + 1).start()

            if a < 2:
                @pl.when(j + 1 == tiles)
                def _():
                    tile_load(a + 1, 0).start()

            @pl.when(t >= 2)
            def _():
                part_copy(t - 2).wait_send()

            @pl.loop(0, half // ROW_BLOCK)
            def _(m):
                part = pl.ds(pl.multiple_of(m * ROW_BLOCK, ROW_BLOCK), ROW_BLOCK)
                theirs = pl.ds(pl.multiple_of((1 - core) * half + m * ROW_BLOCK, ROW_BLOCK), ROW_BLOCK)
                give[s, part] = jnp.dot(flipped[theirs, :], tile[s], preferred_element_type=jnp.float32)

            part_copy(t).start()

            @pl.loop(0, half // ROW_BLOCK)
            def _(m):
                part = pl.ds(pl.multiple_of(m * ROW_BLOCK, ROW_BLOCK), ROW_BLOCK)
                ours = pl.ds(pl.multiple_of(core * half + m * ROW_BLOCK, ROW_BLOCK), ROW_BLOCK)
                mine[part] = jnp.dot(flipped[ours, :], tile[s], preferred_element_type=jnp.float32)

            @pl.when(j >= 3)
            def _():
                shipped(a, j - 3)

            if a == 1:
                @pl.when(j < 3)
                def _():
                    shipped(0, tiles - 3 + j)

            part_copy(t).wait_recv()
            w = lax.rem(j, 3)
            if a == 2:
                total_t[w] = (mine[...] + got[s]).T
            else:
                total[w] = mine[...] + got[s]

            @pl.when(home)
            def _():
                home_copy(a, j).start()

            @pl.when(jnp.logical_not(home))
            def _():
                far_copy(a, j).start()

    for a in (1, 2):
        for j in range(tiles - 3, tiles):
            shipped(a, j)
    for t in range(3 * tiles - 2, 3 * tiles):
        part_copy(t).wait_send()

    @pl.when(jnp.logical_not(home))
    def _():
        for a in range(3):
            remote(targets[a], targets[a], far_send.at[0], far_recv.at[a], swap).wait_recv()


def gradients(n_flat, e_flat, da_flat, db_flat, u_flat):
    tokens, width = n_flat.shape
    hid = da_flat.shape[1]
    half = width // 2
    anywhere = pl.BlockSpec(memory_space=pl.ANY)
    return pl.pallas_call(
        gradient_kernel,
        in_specs=[anywhere] * 5,
        out_specs=[anywhere] * 3,
        out_shape=[jax.ShapeDtypeStruct((half, hid), jnp.float32)] * 2 + [jax.ShapeDtypeStruct((hid, half), jnp.float32)],
        scratch_shapes=[pltpu.VMEM((2, COLS, width), jnp.bfloat16), pltpu.VMEM((width, tokens), jnp.bfloat16), pltpu.VMEM((2, tokens, COLS), jnp.bfloat16),
                        pltpu.VMEM((half, COLS), jnp.float32), pltpu.VMEM((2, half, COLS), jnp.float32), pltpu.VMEM((2, half, COLS), jnp.float32),
                        pltpu.VMEM((3, half, COLS), jnp.float32), pltpu.VMEM((3, COLS, half), jnp.float32)]
        + dma(2, 2, 2, 2, 3, 3, 3, 3, 3),
        cost_estimate=pl.CostEstimate(flops=6 * tokens * width * hid, bytes_accessed=6 * tokens * hid, transcendentals=0),
        compiler_params=pltpu.CompilerParams(has_side_effects=True, vmem_limit_bytes=VMEM_BYTES),
        name="gradients",
    )(n_flat, e_flat, da_flat, db_flat, u_flat)


def solution(mesh):
    fine = Mesh(mesh.devices.reshape(2, 2, 2, 2), ALL_AXES)
    act_spec = P(None, 'dp', 'tp', None)
    up_spec = P(('x', 'core'), None, 'dp', 'tp')
    down_spec = P(('x', 'core'), None, 'tp', 'dp')

    def train_step(x_in, g_out, w_gate, w_in, w_out):
        width = x_in.shape[3]
        x_in_chunks = x_in.reshape(-1, ROWS, width)
        g_in_chunks = g_out.reshape(-1, ROWS, width)
        n_chunks = x_in_chunks.shape[0]

        own = [send(w[0, 0], HOME_SWAP) for w in (w_gate, w_in, w_out)]
        blocks = own + [send(block, ACROSS_CORE) for block in own]
        saved_h, saved_n, _ = forward_phase(x_in_chunks, blocks)
        dx, saved_e, saved_u, saved_da, saved_db, _ = backward_phase(g_in_chunks, saved_h, saved_n, blocks)

        def flat(array):
            return array.reshape(n_chunks * 2 * ROWS, array.shape[-1])

        grads = gradients(flat(saved_n), flat(saved_e), flat(saved_da), flat(saved_db), flat(saved_u))
        dw_gate, dw_in, dw_out = (grad[None, None] for grad in grads)
        return dx.reshape(x_in.shape), dw_gate, dw_in, dw_out

    return jax.shard_map(train_step, mesh=fine, in_specs=(act_spec, act_spec, up_spec, up_spec, down_spec), out_specs=(act_spec, up_spec, up_spec, down_spec), check_vma=False)
```

```python
import jax
import jax.numpy as jnp
from jax import lax
from jax.experimental import pallas as pl
from jax.experimental.pallas import tpu as pltpu
from jax.sharding import Mesh, PartitionSpec as P

RMS_EPS = 1e-6
CONTRACT_ROWS = (((0,), (0,)), ((), ()))
CONTRACT_COLS = (((1,), (1,)), ((), ()))
ALL_AXES = ('tp', 'dp', 'x', 'core')
COLS = 512
ROWS = 64
ROW_BLOCK = 256
DEPTH = 6
EARLY = 6
RELAYED = 4
VMEM_BYTES = 60 * 1024 * 1024

def rms_parts(h_tok):
    h_f32 = h_tok.astype(jnp.float32)
    inv_rms = lax.rsqrt(jnp.mean(h_f32 * h_f32, axis=-1, keepdims=True) + RMS_EPS)
    return h_f32, inv_rms, (h_f32 * inv_rms).astype(jnp.bfloat16)


def swiglu_parts(normed_all, w_gate_l, w_in_l):
    gate_pre = jnp.dot(normed_all, w_gate_l, preferred_element_type=jnp.float32)
    in_pre = jnp.dot(normed_all, w_in_l, preferred_element_type=jnp.float32)
    gate_sig = jax.nn.sigmoid(gate_pre)
    return gate_pre, in_pre, gate_sig, gate_pre * gate_sig


def stage_place():
    z, y, x, core = (lax.axis_index(name) for name in ALL_AXES)
    after = {'dp': 1 - y, 'x': x + y}
    before = {'dp': 1 - y, 'x': x + y - 1}
    return 2 * x + y, core, {'tp': 1 - z}, after, before


def remote(source, target, send_sem, recv_sem, place):
    return pltpu.make_async_remote_copy(src_ref=source, dst_ref=target, send_sem=send_sem, recv_sem=recv_sem, device_id=place, device_id_type=pl.DeviceIdType.MESH)


def forward_kernel(x_ref, *refs):
    own = refs[:3]
    saved_h, saved_n, x_land = refs[3:6]
    kept = refs[6:9]
    (w_gate, w_in, w_out, h_buf, n_own, n_peer, acc, keep, give, got, h_out,
     w_sem, load_sem, h_send, h_recv, n_send, n_recv, g_send, g_recv, save_h, save_own, save_peer, far_send, far_recv, relay, b_send, b_recv, free) = refs[9:]
    n = x_ref.shape[0]
    rows = x_ref.shape[1]
    hid = w_gate.shape[1]
    stage, core, peer, after, before = stage_place()
    y, x = lax.axis_index('dp'), lax.axis_index('x')
    half = own[0].shape[0]
    direct = hid - hid // RELAYED
    short = stage == 0
    home = core == y

    def mine(k, low, size):
        return own[k].at[pl.ds(low, size), :] if k == 2 else own[k].at[:, pl.ds(low, size)]

    def spot(k, which, low, size):
        part = pl.ds(pl.multiple_of(which * half, half), half)
        return w_out.at[pl.ds(low, size), part] if k == 2 else (w_gate, w_in)[k].at[part, pl.ds(low, size)]

    def local_block(k):
        return pltpu.make_async_copy(mine(k, 0, hid), spot(k, y, 0, hid), w_sem.at[k])

    def block_copy(k, kind, source, target, place):
        return remote(source, target, b_send.at[kind, k], b_recv.at[kind, k], place)

    def partner_block(k):
        return block_copy(k, 0, mine(k, 0, hid), spot(k, y, 0, hid), {'core': 1 - core})

    def away_block(k, size):
        return block_copy(k, 1, mine(k, 0, size), spot(k, y, 0, size), {'dp': 1 - y, 'core': 1 - core})

    def shared_block(k):
        return block_copy(k, 2, spot(k, 1 - y, 0, hid), spot(k, 1 - y, 0, hid), {'core': 1 - core})

    def hop(k, number):
        rest = hid - direct
        source = mine(k, direct, rest) if number == 0 else relay.at[k]
        target = spot(k, 1, direct, rest) if number == 2 else relay.at[k]
        place = ({'x': 1, 'core': 1}, {'dp': 0, 'core': 0}, {'x': 0, 'core': 1})[number]
        return block_copy(k, 3, source, target, place)

    hop_from = ((stage == 1) & (core == 0), (stage == 3) & (core == 1), (stage == 2) & (core == 0))

    @pl.when(home)
    def _():
        for k in range(3):
            partner_block(k).start()
            local_block(k).start()

    @pl.when(jnp.logical_not(home) & (stage == 1))
    def _():
        for k in range(3):
            hop(k, 0).start()
            away_block(k, direct).start()

    @pl.when(jnp.logical_not(home) & (stage != 1))
    def _():
        for k in range(3):
            away_block(k, hid).start()

    for number in (1, 2):
        @pl.when(hop_from[number])
        def _(number=number):
            for k in range(3):
                hop(k, number - 1).wait_recv()
                hop(k, number).start()

    def weights_ready():
        @pl.when(home)
        def _():
            for k in range(3):
                local_block(k).wait()
                shared_block(k).wait_recv()

        @pl.when(jnp.logical_not(home))
        def _():
            for k in range(3):
                @pl.when(short)
                def _():
                    away_block(k, direct).wait_recv()
                    hop(k, 2).wait_recv()

                @pl.when(jnp.logical_not(short))
                def _():
                    away_block(k, hid).wait_recv()

                shared_block(k).start()
            for k in range(3):
                partner_block(k).wait_recv()

        for k in range(3):
            keep_weight(k).start()

    def keep_weight(k):
        return pltpu.make_async_copy((w_gate, w_in, w_out)[k], kept[k], w_sem.at[3 + k])

    def push(low, high):
        @pl.when((stage == 1) & (core == 1))
        def _():
            @pl.loop(low, high)
            def _(c):
                far_copy(c).start()

    def x_load(c, source):
        return pltpu.make_async_copy(source.at[c], h_buf.at[lax.rem(c, DEPTH)], load_sem.at[lax.rem(c, 2)])

    def far_copy(c):
        return remote(x_ref.at[c], x_land.at[c], far_send.at[c], far_recv.at[c], {'dp': 0})

    def start_load(c):
        @pl.when(core == 0)
        def _():
            x_load(c, x_ref).start()

        @pl.when(core == 1)
        def _():
            far_copy(c).wait_recv()
            x_load(c, x_land).start()

    push(0, EARLY)

    @pl.when(stage > 0)
    def _():
        weights_ready()

    def h_copy(c):
        return remote(h_out.at[lax.rem(c, 2)], h_buf.at[lax.rem(c, DEPTH)], h_send.at[lax.rem(c, 2)], h_recv.at[lax.rem(c, DEPTH)], after)

    def n_copy(c):
        s = lax.rem(c, 4)
        return remote(n_own.at[s], n_peer.at[s], n_send.at[s], n_recv.at[s], peer)

    def give_copy(c):
        s = lax.rem(c, 3)
        return remote(give.at[s], got.at[s], g_send.at[s], g_recv.at[s], peer)

    def keep_h(c):
        s = lax.rem(c, DEPTH)
        return pltpu.make_async_copy(h_buf.at[s], saved_h.at[c], save_h.at[s])

    def keep_own(c):
        s = lax.rem(c, 4)
        return pltpu.make_async_copy(n_own.at[s], saved_n.at[c, pl.ds(0, rows)], save_own.at[s])

    def keep_peer(c):
        s = lax.rem(c, 4)
        return pltpu.make_async_copy(n_peer.at[s], saved_n.at[c, pl.ds(rows, rows)], save_peer.at[s])

    @pl.when(stage == 0)
    def _():
        start_load(0)

    def body(i, carry):
        @pl.when(i < n)
        def _():
            @pl.when(stage == 0)
            def _():
                x_load(i, x_ref).wait()

                @pl.when(i + 1 < n)
                def _():
                    start_load(i + 1)

            @pl.when(stage > 0)
            def _():
                h_copy(i).wait_recv()

            keep_h(i).start()

            @pl.when(i >= 4)
            def _():
                n_copy(i - 4).wait_send()
                keep_own(i - 4).wait()

            n_own[lax.rem(i, 4)] = rms_parts(h_buf[lax.rem(i, DEPTH)])[2]
            n_copy(i).start()
            keep_own(i).start()

        @pl.when(i == 0)
        def _():
            push(EARLY, n)

        @pl.when((i == 1) & (stage == 0))
        def _():
            weights_ready()

        @pl.when((i >= 1) & (i <= n))
        def _():
            c = i - 1
            s = lax.rem(c, 3)
            n_copy(c).wait_recv()
            keep_peer(c).start()
            @pl.when(stage < 3)
            def _():
                both = jnp.concatenate([n_own[lax.rem(c, 4)], n_peer[lax.rem(c, 4)]], 0)
                for j in range(hid // COLS):
                    part = pl.ds(j * COLS, COLS)
                    gate_pre, in_pre, gate_sig, gate_act = swiglu_parts(both, w_gate[:, part], w_in[:, part])
                    branch = jnp.dot((gate_act * in_pre).astype(jnp.bfloat16), w_out[part, :], preferred_element_type=jnp.float32)
                    acc[...] = branch if j == 0 else acc[...] + branch
                keep[s] = acc[:rows]
                give[s] = acc[rows:]

            keep_peer(c).wait()

            @pl.when(stage < 3)
            def _():
                give_copy(c).start()

        @pl.when(i >= 2)
        def _():
            c = i - 2
            s = lax.rem(c, 3)
            keep_h(c).wait()

            @pl.when(stage < 3)
            def _():
                give_copy(c).wait_recv()
                give_copy(c).wait_send()

                @pl.when(c >= 2)
                def _():
                    h_copy(c - 2).wait_send()

                h_out[lax.rem(c, 2)] = h_buf[lax.rem(c, DEPTH)] + (keep[s] + got[s]).astype(jnp.bfloat16)

                @pl.when(c >= DEPTH)
                def _():
                    pl.semaphore_wait(free, 1)

                h_copy(c).start()

            @pl.when((stage > 0) & (c < n - DEPTH))
            def _():
                pl.semaphore_signal(free, inc=1, device_id=before, device_id_type=pl.DeviceIdType.MESH)

        return carry

    lax.fori_loop(0, n + 2, body, 0)
    for c in range(n - 4, n):
        n_copy(c).wait_send()
        keep_own(c).wait()

    @pl.when((stage == 1) & (core == 1))
    def _():
        @pl.loop(0, n)
        def _(c):
            far_copy(c).wait_send()

    for number in range(3):
        @pl.when(hop_from[number])
        def _(number=number):
            for k in range(3):
                hop(k, number).wait_send()

    for k in range(3):
        keep_weight(k).wait()

        @pl.when(home)
        def _():
            partner_block(k).wait_send()

        @pl.when(jnp.logical_not(home))
        def _():
            shared_block(k).wait_send()

            @pl.when(stage == 1)
            def _():
                away_block(k, direct).wait_send()

            @pl.when(stage != 1)
            def _():
                away_block(k, hid).wait_send()

    @pl.when(stage < 3)
    def _():
        for c in range(n - 2, n):
            h_copy(c).wait_send()


def backward_kernel(g_ref, saved_h, saved_n, *refs):
    kept = refs[:3]
    dx_ref, saved_e, saved_u, saved_da, saved_db, g_land = refs[3:9]
    (w_gate, w_in, w_out, e_buf, e_peer, n_buf, h_buf, acc, keep, give, got, e_out, u_out, da_out, db_out,
     w_sem, load_sem, n_sem, h_sem, s_send, s_recv, e_send, e_recv, g_send, g_recv, save_own, save_peer, save_u, save_da, save_db, dx_sem, dx_send, dx_recv, far_send, far_recv, free) = refs[9:]
    n = g_ref.shape[0]
    rows = g_ref.shape[1]
    hid = w_gate.shape[1]
    stage, core, peer, after, before = stage_place()
    loads = [pltpu.make_async_copy(kept[k], (w_gate, w_in, w_out)[k], w_sem.at[k]) for k in range(3)]
    for load in loads:
        load.start()

    def g_load(c, source):
        return pltpu.make_async_copy(source.at[c], e_buf.at[lax.rem(c, DEPTH)], load_sem.at[lax.rem(c, 2)])

    def far_copy(c):
        return remote(g_ref.at[c], g_land.at[c], far_send.at[c], far_recv.at[c], {'dp': 1})

    def start_load(c):
        @pl.when(core == 1)
        def _():
            g_load(c, g_ref).start()

        @pl.when(core == 0)
        def _():
            far_copy(c).wait_recv()
            g_load(c, g_land).start()

    @pl.when((stage == 2) & (core == 0))
    def _():
        @pl.loop(0, n)
        def _(c):
            far_copy(c).start()

    def n_load(c):
        s = lax.rem(c, 3)
        return pltpu.make_async_copy(saved_n.at[c], n_buf.at[s], n_sem.at[s])

    def h_load(c):
        s = lax.rem(c, 3)
        return pltpu.make_async_copy(saved_h.at[c], h_buf.at[s], h_sem.at[s])

    def stage_copy(c):
        return remote(e_out.at[lax.rem(c, 2)], e_buf.at[lax.rem(c, DEPTH)], s_send.at[lax.rem(c, 2)], s_recv.at[lax.rem(c, DEPTH)], before)

    def e_copy(c):
        s = lax.rem(c, 3)
        return remote(e_buf.at[lax.rem(c, DEPTH)], e_peer.at[s], e_send.at[s], e_recv.at[s], peer)

    def give_copy(c):
        s = lax.rem(c, 3)
        return remote(give.at[s], got.at[s], g_send.at[s], g_recv.at[s], peer)

    def keep_own(c):
        return pltpu.make_async_copy(e_buf.at[lax.rem(c, DEPTH)], saved_e.at[c, pl.ds(0, rows)], save_own.at[lax.rem(c, 3)])

    def keep_peer(c):
        s = lax.rem(c, 3)
        return pltpu.make_async_copy(e_peer.at[s], saved_e.at[c, pl.ds(rows, rows)], save_peer.at[s])

    def keep_wide(c):
        s = lax.rem(c, 2)
        return [pltpu.make_async_copy(source.at[s], target.at[c], sem.at[s])
                for source, target, sem in ((u_out, saved_u, save_u), (da_out, saved_da, save_da), (db_out, saved_db, save_db))]

    def keep_dx(c):
        s = lax.rem(c, 2)
        return pltpu.make_async_copy(e_out.at[s], dx_ref.at[c], dx_sem.at[s])

    def dx_copy(c, k):
        s = lax.rem(c, 2)
        return remote(e_out.at[s], dx_ref.at[c], dx_send.at[s, k], dx_recv.at[0], {'dp': core, 'x': k // 2, 'core': k % 2})

    def dx_start(c):
        @pl.when(core == 0)
        def _():
            keep_dx(c).start()

        @pl.when(core == 1)
        def _():
            dx_copy(c, 0).start()

        for k in range(1, 4):
            dx_copy(c, k).start()

    def dx_done(c):
        @pl.when(core == 0)
        def _():
            keep_dx(c).wait()

        @pl.when(core == 1)
        def _():
            dx_copy(c, 0).wait_send()

        for k in range(1, 4):
            dx_copy(c, k).wait_send()

    @pl.when(stage == 3)
    def _():
        start_load(0)

    def body(i, carry):
        @pl.when(i < n)
        def _():
            n_load(i).start()
            h_load(i).start()

            @pl.when(stage == 3)
            def _():
                g_load(i, g_ref).wait()

                @pl.when(i + 1 < n)
                def _():
                    start_load(i + 1)

            @pl.when(stage < 3)
            def _():
                stage_copy(i).wait_recv()

            e_copy(i).start()
            keep_own(i).start()

        @pl.when(i == 1)
        def _():
            for load in loads:
                load.wait()

        @pl.when((i >= 1) & (i <= n))
        def _():
            c = i - 1
            s = lax.rem(c, 3)
            w = lax.rem(c, 2)
            n_load(c).wait()
            e_copy(c).wait_recv()
            keep_peer(c).start()

            @pl.when(c >= 2)
            def _():
                for copy in keep_wide(c - 2):
                    copy.wait()

            normed = n_buf[s]
            both = jnp.concatenate([e_buf[lax.rem(c, DEPTH)], e_peer[s]], 0)
            for j in range(hid // COLS):
                part = pl.ds(j * COLS, COLS)
                gate_pre, in_pre, gate_sig, gate_act = swiglu_parts(normed, w_gate[:, part], w_in[:, part])
                d_hidden = lax.dot_general(both, w_out[part, :], CONTRACT_COLS, preferred_element_type=jnp.float32).astype(jnp.bfloat16).astype(jnp.float32)
                u_out[w, :, part] = (gate_act * in_pre).astype(jnp.bfloat16)
                d_gate = (d_hidden * in_pre * (gate_sig * (1.0 + gate_pre * (1.0 - gate_sig)))).astype(jnp.bfloat16)
                d_up = (d_hidden * gate_act).astype(jnp.bfloat16)
                da_out[w, :, part] = d_gate
                db_out[w, :, part] = d_up
            for copy in keep_wide(c):
                copy.start()
            acc[...] = lax.dot_general(da_out[w], w_gate[...], CONTRACT_COLS, preferred_element_type=jnp.float32) + lax.dot_general(db_out[w], w_in[...], CONTRACT_COLS, preferred_element_type=jnp.float32)
            keep[s] = acc[:rows]
            give[s] = acc[rows:]
            keep_peer(c).wait()
            give_copy(c).start()

        @pl.when(i >= 2)
        def _():
            c = i - 2
            s = lax.rem(c, 3)
            w = lax.rem(c, 2)
            h_load(c).wait()
            give_copy(c).wait_recv()
            give_copy(c).wait_send()
            e_copy(c).wait_send()
            keep_own(c).wait()

            @pl.when(c >= 2)
            def _():
                @pl.when(stage > 0)
                def _():
                    stage_copy(c - 2).wait_send()

                @pl.when(stage == 0)
                def _():
                    dx_done(c - 2)

            d_norm = keep[s] + got[s]
            h_f32, inv_rms, _ = rms_parts(h_buf[s])
            unit_rms = h_f32 * inv_rms
            d_h = inv_rms * (d_norm - unit_rms * jnp.mean(d_norm * unit_rms, axis=-1, keepdims=True))
            e_out[w] = (e_buf[lax.rem(c, DEPTH)].astype(jnp.float32) + d_h).astype(jnp.bfloat16)

            @pl.when(stage > 0)
            def _():
                @pl.when(c >= DEPTH)
                def _():
                    pl.semaphore_wait(free, 1)

                stage_copy(c).start()

            @pl.when(stage == 0)
            def _():
                dx_start(c)

            @pl.when((stage < 3) & (c < n - DEPTH))
            def _():
                pl.semaphore_signal(free, inc=1, device_id=after, device_id_type=pl.DeviceIdType.MESH)

        return carry

    lax.fori_loop(0, n + 2, body, 0)
    for c in range(n - 2, n):
        for copy in keep_wide(c):
            copy.wait()

        @pl.when(stage > 0)
        def _():
            stage_copy(c).wait_send()

        @pl.when(stage == 0)
        def _():
            dx_done(c)

    @pl.when((stage > 0) | (core > 0))
    def _():
        remote(dx_ref, dx_ref, dx_send.at[0, 0], dx_recv.at[0], peer).wait_recv()

    @pl.when((stage == 2) & (core == 0))
    def _():
        @pl.loop(0, n)
        def _(c):
            far_copy(c).wait_send()


def common_scratch(width, hid, rows):
    return [pltpu.VMEM((width, hid), jnp.bfloat16), pltpu.VMEM((width, hid), jnp.bfloat16), pltpu.VMEM((hid, width), jnp.bfloat16),
            pltpu.VMEM((DEPTH, rows, width), jnp.bfloat16)]


def partial_scratch(width, rows):
    return [pltpu.VMEM((2 * rows, width), jnp.float32)] + [pltpu.VMEM((3, rows, width), jnp.float32)] * 3 + [pltpu.VMEM((2, rows, width), jnp.bfloat16)]


def dma(*sizes):
    return [pltpu.SemaphoreType.DMA((size,)) for size in sizes]


def forward_phase(x_chunks, blocks):
    n, rows, width = x_chunks.shape
    half, hid = blocks[0].shape
    whole = [jax.ShapeDtypeStruct((width, hid), jnp.bfloat16)] * 2 + [jax.ShapeDtypeStruct((hid, width), jnp.bfloat16)]
    anywhere = pl.BlockSpec(memory_space=pl.ANY)
    return pl.pallas_call(
        forward_kernel,
        in_specs=[anywhere] * 4,
        out_specs=[anywhere] * 6,
        out_shape=[jax.ShapeDtypeStruct((n, rows, width), jnp.bfloat16), jax.ShapeDtypeStruct((n, 2 * rows, width), jnp.bfloat16), jax.ShapeDtypeStruct((n, rows, width), jnp.bfloat16)] + whole,
        scratch_shapes=common_scratch(width, hid, rows) + [pltpu.VMEM((4, rows, width), jnp.bfloat16)] * 2 + partial_scratch(width, rows)
        + dma(6, 2, 2, DEPTH, 4, 4, 3, 3, DEPTH, 4, 4, n, n)
        + [pltpu.VMEM((3, half, hid // RELAYED), jnp.bfloat16), pltpu.SemaphoreType.DMA((4, 3)), pltpu.SemaphoreType.DMA((4, 3))] + [pltpu.SemaphoreType.REGULAR],
        cost_estimate=pl.CostEstimate(flops=12 * n * rows * width * hid, bytes_accessed=6 * width * hid, transcendentals=0),
        compiler_params=pltpu.CompilerParams(has_side_effects=True, vmem_limit_bytes=VMEM_BYTES),
        name="forward_phase",
    )(x_chunks, *blocks)


def backward_phase(g_chunks, saved_h, saved_n, blocks):
    n, rows, width = g_chunks.shape
    hid = blocks[0].shape[1]
    anywhere = pl.BlockSpec(memory_space=pl.ANY)
    wide = jax.ShapeDtypeStruct((n, 2 * rows, hid), jnp.bfloat16)
    return pl.pallas_call(
        backward_kernel,
        in_specs=[anywhere] * 6,
        out_specs=[anywhere] * 6,
        out_shape=[jax.ShapeDtypeStruct((n, rows, width), jnp.bfloat16), jax.ShapeDtypeStruct((n, 2 * rows, width), jnp.bfloat16), wide, wide, wide, jax.ShapeDtypeStruct((n, rows, width), jnp.bfloat16)],
        scratch_shapes=common_scratch(width, hid, rows)
        + [pltpu.VMEM((3, rows, width), jnp.bfloat16), pltpu.VMEM((3, 2 * rows, width), jnp.bfloat16), pltpu.VMEM((3, rows, width), jnp.bfloat16)]
        + partial_scratch(width, rows) + [pltpu.VMEM((2, 2 * rows, hid), jnp.bfloat16)] * 3
        + dma(3, 2, 3, 3, 2, DEPTH, 3, 3, 3, 3, 3, 3, 2, 2, 2, 2) + [pltpu.SemaphoreType.DMA((2, 4))] + dma(1, n, n) + [pltpu.SemaphoreType.REGULAR],
        cost_estimate=pl.CostEstimate(flops=20 * n * rows * width * hid, bytes_accessed=6 * width * hid, transcendentals=0),
        compiler_params=pltpu.CompilerParams(has_side_effects=True, vmem_limit_bytes=VMEM_BYTES),
        name="backward_phase",
    )(g_chunks, saved_h, saved_n, *blocks)


def gradient_kernel(n_ref, e_ref, da_ref, db_ref, u_ref, dw_gate, dw_in, dw_out,
                    raw, flipped, tile, mine, give, got, total, total_t,
                    raw_sem, tile_sem, p_send, p_recv, keep_sem, keep_t_sem, far_send, far_t_send, far_recv):
    z, y, x, core = (lax.axis_index(name) for name in ALL_AXES)
    tokens, width = n_ref.shape
    hid = da_ref.shape[1]
    half = width // 2
    tiles = hid // COLS
    steps = tokens // COLS
    home = core == y
    swap = {'dp': 1 - y, 'core': 1 - core}
    sources = (da_ref, db_ref, u_ref)
    targets = (dw_gate, dw_in, dw_out)

    def cols(j):
        return pl.ds(pl.multiple_of(j * COLS, COLS), COLS)

    def raw_load(source, k):
        return pltpu.make_async_copy(source.at[cols(k)], raw.at[lax.rem(k, 2)], raw_sem.at[lax.rem(k, 2)])

    def tile_load(a, j):
        s = lax.rem(a * tiles + j, 2)
        return pltpu.make_async_copy(sources[a].at[:, cols(j)], tile.at[s], tile_sem.at[s])

    def part_copy(t):
        s = lax.rem(t, 2)
        return remote(give.at[s], got.at[s], p_send.at[s], p_recv.at[s], {'core': 1 - core})

    def place(a, j):
        return (total_t if a == 2 else total).at[lax.rem(j, 3)], (targets[a].at[cols(j)] if a == 2 else targets[a].at[:, cols(j)])

    def home_copy(a, j):
        source, target = place(a, j)
        return pltpu.make_async_copy(source, target, (keep_t_sem if a == 2 else keep_sem).at[lax.rem(j, 3)])

    def far_copy(a, j):
        source, target = place(a, j)
        return remote(source, target, (far_t_send if a == 2 else far_send).at[lax.rem(j, 3)], far_recv.at[a], swap)

    def shipped(a, j):
        @pl.when(home)
        def _():
            home_copy(a, j).wait()

        @pl.when(jnp.logical_not(home))
        def _():
            far_copy(a, j).wait_send()

    def flip(source):
        raw_load(source, 0).start()

        @pl.loop(0, steps)
        def _(k):
            raw_load(source, k).wait()

            @pl.when(k + 1 < steps)
            def _():
                raw_load(source, k + 1).start()

            flipped[:, cols(k)] = raw[lax.rem(k, 2)].T

    tile_load(0, 0).start()
    for a in range(3):
        if a != 1:
            flip(n_ref if a == 0 else e_ref)

        @pl.loop(0, tiles)
        def _(j, a=a):
            t = a * tiles + j
            s = lax.rem(t, 2)
            tile_load(a, j).wait()

            @pl.when(j + 1 < tiles)
            def _():
                tile_load(a, j + 1).start()

            if a < 2:
                @pl.when(j + 1 == tiles)
                def _():
                    tile_load(a + 1, 0).start()

            @pl.when(t >= 2)
            def _():
                part_copy(t - 2).wait_send()

            @pl.loop(0, half // ROW_BLOCK)
            def _(m):
                part = pl.ds(pl.multiple_of(m * ROW_BLOCK, ROW_BLOCK), ROW_BLOCK)
                theirs = pl.ds(pl.multiple_of((1 - core) * half + m * ROW_BLOCK, ROW_BLOCK), ROW_BLOCK)
                give[s, part] = jnp.dot(flipped[theirs, :], tile[s], preferred_element_type=jnp.float32)

            part_copy(t).start()

            @pl.loop(0, half // ROW_BLOCK)
            def _(m):
                part = pl.ds(pl.multiple_of(m * ROW_BLOCK, ROW_BLOCK), ROW_BLOCK)
                ours = pl.ds(pl.multiple_of(core * half + m * ROW_BLOCK, ROW_BLOCK), ROW_BLOCK)
                mine[part] = jnp.dot(flipped[ours, :], tile[s], preferred_element_type=jnp.float32)

            @pl.when(j >= 3)
            def _():
                shipped(a, j - 3)

            if a == 1:
                @pl.when(j < 3)
                def _():
                    shipped(0, tiles - 3 + j)

            part_copy(t).wait_recv()
            w = lax.rem(j, 3)
            if a == 2:
                total_t[w] = (mine[...] + got[s]).T
            else:
                total[w] = mine[...] + got[s]

            @pl.when(home)
            def _():
                home_copy(a, j).start()

            @pl.when(jnp.logical_not(home))
            def _():
                far_copy(a, j).start()

    for a in (1, 2):
        for j in range(tiles - 3, tiles):
            shipped(a, j)
    for t in range(3 * tiles - 2, 3 * tiles):
        part_copy(t).wait_send()

    @pl.when(jnp.logical_not(home))
    def _():
        for a in range(3):
            remote(targets[a], targets[a], far_send.at[0], far_recv.at[a], swap).wait_recv()


def gradients(n_flat, e_flat, da_flat, db_flat, u_flat):
    tokens, width = n_flat.shape
    hid = da_flat.shape[1]
    half = width // 2
    anywhere = pl.BlockSpec(memory_space=pl.ANY)
    return pl.pallas_call(
        gradient_kernel,
        in_specs=[anywhere] * 5,
        out_specs=[anywhere] * 3,
        out_shape=[jax.ShapeDtypeStruct((half, hid), jnp.float32)] * 2 + [jax.ShapeDtypeStruct((hid, half), jnp.float32)],
        scratch_shapes=[pltpu.VMEM((2, COLS, width), jnp.bfloat16), pltpu.VMEM((width, tokens), jnp.bfloat16), pltpu.VMEM((2, tokens, COLS), jnp.bfloat16),
                        pltpu.VMEM((half, COLS), jnp.float32), pltpu.VMEM((2, half, COLS), jnp.float32), pltpu.VMEM((2, half, COLS), jnp.float32),
                        pltpu.VMEM((3, half, COLS), jnp.float32), pltpu.VMEM((3, COLS, half), jnp.float32)]
        + dma(2, 2, 2, 2, 3, 3, 3, 3, 3),
        cost_estimate=pl.CostEstimate(flops=6 * tokens * width * hid, bytes_accessed=6 * tokens * hid, transcendentals=0),
        compiler_params=pltpu.CompilerParams(has_side_effects=True, vmem_limit_bytes=VMEM_BYTES),
        name="gradients",
    )(n_flat, e_flat, da_flat, db_flat, u_flat)


def solution(mesh):
    fine = Mesh(mesh.devices.reshape(2, 2, 2, 2), ALL_AXES)
    act_spec = P(None, 'dp', 'tp', None)
    up_spec = P(('x', 'core'), None, 'dp', 'tp')
    down_spec = P(('x', 'core'), None, 'tp', 'dp')

    def train_step(x_in, g_out, w_gate, w_in, w_out):
        width = x_in.shape[3]
        x_in_chunks = x_in.reshape(-1, ROWS, width)
        g_in_chunks = g_out.reshape(-1, ROWS, width)
        n_chunks = x_in_chunks.shape[0]

        saved_h, saved_n, _, *weights = forward_phase(x_in_chunks, [w[0, 0] for w in (w_gate, w_in, w_out)])
        dx, saved_e, saved_u, saved_da, saved_db, _ = backward_phase(g_in_chunks, saved_h, saved_n, weights)

        def flat(array):
            return array.reshape(n_chunks * 2 * ROWS, array.shape[-1])

        grads = gradients(flat(saved_n), flat(saved_e), flat(saved_da), flat(saved_db), flat(saved_u))
        dw_gate, dw_in, dw_out = (grad[None, None] for grad in grads)
        return dx.reshape(x_in.shape), dw_gate, dw_in, dw_out

    return jax.shard_map(train_step, mesh=fine, in_specs=(act_spec, act_spec, up_spec, up_spec, down_spec), out_specs=(act_spec, up_spec, up_spec, down_spec), check_vma=False)
```

```python
import jax
import jax.numpy as jnp
from jax import lax
from jax.experimental import pallas as pl
from jax.experimental.pallas import tpu as pltpu
from jax.sharding import Mesh, PartitionSpec as P

RMS_EPS = 1e-6
CONTRACT_ROWS = (((0,), (0,)), ((), ()))
CONTRACT_COLS = (((1,), (1,)), ((), ()))
ALL_AXES = ('tp', 'dp', 'x', 'core')
COLS = 512
ROWS = 64
ROW_BLOCK = 256
DEPTH = 6
EARLY = 6
RELAYED = 4
VMEM_BYTES = 60 * 1024 * 1024

def rms_parts(h_tok):
    h_f32 = h_tok.astype(jnp.float32)
    inv_rms = lax.rsqrt(jnp.mean(h_f32 * h_f32, axis=-1, keepdims=True) + RMS_EPS)
    return h_f32, inv_rms, (h_f32 * inv_rms).astype(jnp.bfloat16)


def swiglu_parts(normed_all, w_gate_l, w_in_l):
    gate_pre = jnp.dot(normed_all, w_gate_l, preferred_element_type=jnp.float32)
    in_pre = jnp.dot(normed_all, w_in_l, preferred_element_type=jnp.float32)
    gate_sig = jax.nn.sigmoid(gate_pre)
    return gate_pre, in_pre, gate_sig, gate_pre * gate_sig


def stage_place():
    z, y, x, core = (lax.axis_index(name) for name in ALL_AXES)
    after = {'dp': 1 - y, 'x': x + y}
    before = {'dp': 1 - y, 'x': x + y - 1}
    return 2 * x + y, core, {'tp': 1 - z}, after, before


def remote(source, target, send_sem, recv_sem, place):
    return pltpu.make_async_remote_copy(src_ref=source, dst_ref=target, send_sem=send_sem, recv_sem=recv_sem, device_id=place, device_id_type=pl.DeviceIdType.MESH)


def forward_kernel(x_ref, *refs):
    own = refs[:3]
    saved_h, saved_n, x_land = refs[3:6]
    kept = refs[6:9]
    kept_t = refs[9]
    (w_gate, w_in, w_out, h_buf, n_own, n_peer, acc, keep, give, got, h_out,
     w_sem, load_sem, h_send, h_recv, n_send, n_recv, g_send, g_recv, save_h, save_own, save_peer, far_send, far_recv, relay, flipped, b_send, b_recv, free) = refs[10:]
    n = x_ref.shape[0]
    rows = x_ref.shape[1]
    hid = w_gate.shape[1]
    stage, core, peer, after, before = stage_place()
    y, x = lax.axis_index('dp'), lax.axis_index('x')
    half = own[0].shape[0]
    direct = hid - hid // RELAYED
    short = stage == 0
    home = core == y

    def mine(k, low, size):
        return own[k].at[pl.ds(low, size), :] if k == 2 else own[k].at[:, pl.ds(low, size)]

    def spot(k, which, low, size):
        part = pl.ds(pl.multiple_of(which * half, half), half)
        return w_out.at[pl.ds(low, size), part] if k == 2 else (w_gate, w_in)[k].at[part, pl.ds(low, size)]

    def local_block(k):
        return pltpu.make_async_copy(mine(k, 0, hid), spot(k, y, 0, hid), w_sem.at[k])

    def block_copy(k, kind, source, target, place):
        return remote(source, target, b_send.at[kind, k], b_recv.at[kind, k], place)

    def partner_block(k):
        return block_copy(k, 0, mine(k, 0, hid), spot(k, y, 0, hid), {'core': 1 - core})

    def away_block(k, size):
        return block_copy(k, 1, mine(k, 0, size), spot(k, y, 0, size), {'dp': 1 - y, 'core': 1 - core})

    def shared_block(k):
        return block_copy(k, 2, spot(k, 1 - y, 0, hid), spot(k, 1 - y, 0, hid), {'core': 1 - core})

    def hop(k, number):
        rest = hid - direct
        source = mine(k, direct, rest) if number == 0 else relay.at[k]
        target = spot(k, 1, direct, rest) if number == 2 else relay.at[k]
        place = ({'x': 1, 'core': 1}, {'dp': 0, 'core': 0}, {'x': 0, 'core': 1})[number]
        return block_copy(k, 3, source, target, place)

    hop_from = ((stage == 1) & (core == 0), (stage == 3) & (core == 1), (stage == 2) & (core == 0))

    @pl.when(home)
    def _():
        for k in range(3):
            partner_block(k).start()
            local_block(k).start()

    @pl.when(jnp.logical_not(home) & (stage == 1))
    def _():
        for k in range(3):
            hop(k, 0).start()
            away_block(k, direct).start()

    @pl.when(jnp.logical_not(home) & (stage != 1))
    def _():
        for k in range(3):
            away_block(k, hid).start()

    for number in (1, 2):
        @pl.when(hop_from[number])
        def _(number=number):
            for k in range(3):
                hop(k, number - 1).wait_recv()
                hop(k, number).start()

    def weights_ready():
        @pl.when(home)
        def _():
            for k in range(3):
                local_block(k).wait()
                shared_block(k).wait_recv()

        @pl.when(jnp.logical_not(home))
        def _():
            for k in range(3):
                @pl.when(short)
                def _():
                    away_block(k, direct).wait_recv()
                    hop(k, 2).wait_recv()

                @pl.when(jnp.logical_not(short))
                def _():
                    away_block(k, hid).wait_recv()

                shared_block(k).start()
            for k in range(3):
                partner_block(k).wait_recv()

        for k in range(3):
            keep_weight(k).start()

    def keep_weight(k):
        return pltpu.make_async_copy((w_gate, w_in, w_out)[k], kept[k], w_sem.at[3 + k])

    def push(low, high):
        @pl.when((stage == 1) & (core == 1))
        def _():
            @pl.loop(low, high)
            def _(c):
                far_copy(c).start()

    def x_load(c, source):
        return pltpu.make_async_copy(source.at[c], h_buf.at[lax.rem(c, DEPTH)], load_sem.at[lax.rem(c, 2)])

    def far_copy(c):
        return remote(x_ref.at[c], x_land.at[c], far_send.at[c], far_recv.at[c], {'dp': 0})

    def start_load(c):
        @pl.when(core == 0)
        def _():
            x_load(c, x_ref).start()

        @pl.when(core == 1)
        def _():
            far_copy(c).wait_recv()
            x_load(c, x_land).start()

    push(0, EARLY)

    @pl.when(stage > 0)
    def _():
        weights_ready()

    keep_flipped = pltpu.make_async_copy(flipped, kept_t, w_sem.at[6])

    @pl.when(stage == 3)
    def _():
        @pl.loop(0, hid // COLS)
        def _(k):
            part = pl.ds(pl.multiple_of(k * COLS, COLS), COLS)
            flipped[:, part] = w_out[part, :].T

        keep_flipped.start()

    def h_copy(c):
        return remote(h_out.at[lax.rem(c, 2)], h_buf.at[lax.rem(c, DEPTH)], h_send.at[lax.rem(c, 2)], h_recv.at[lax.rem(c, DEPTH)], after)

    def n_copy(c):
        s = lax.rem(c, 4)
        return remote(n_own.at[s], n_peer.at[s], n_send.at[s], n_recv.at[s], peer)

    def give_copy(c):
        s = lax.rem(c, 3)
        return remote(give.at[s], got.at[s], g_send.at[s], g_recv.at[s], peer)

    def keep_h(c):
        s = lax.rem(c, DEPTH)
        return pltpu.make_async_copy(h_buf.at[s], saved_h.at[c], save_h.at[s])

    def keep_own(c):
        s = lax.rem(c, 4)
        return pltpu.make_async_copy(n_own.at[s], saved_n.at[c, pl.ds(0, rows)], save_own.at[s])

    def keep_peer(c):
        s = lax.rem(c, 4)
        return pltpu.make_async_copy(n_peer.at[s], saved_n.at[c, pl.ds(rows, rows)], save_peer.at[s])

    @pl.when(stage == 0)
    def _():
        start_load(0)

    def body(i, carry):
        @pl.when(i < n)
        def _():
            @pl.when(stage == 0)
            def _():
                x_load(i, x_ref).wait()

                @pl.when(i + 1 < n)
                def _():
                    start_load(i + 1)

            @pl.when(stage > 0)
            def _():
                h_copy(i).wait_recv()

            keep_h(i).start()

            @pl.when(i >= 4)
            def _():
                n_copy(i - 4).wait_send()
                keep_own(i - 4).wait()

            n_own[lax.rem(i, 4)] = rms_parts(h_buf[lax.rem(i, DEPTH)])[2]
            n_copy(i).start()
            keep_own(i).start()

        @pl.when(i == 0)
        def _():
            push(EARLY, n)

        @pl.when((i == 1) & (stage == 0))
        def _():
            weights_ready()

        @pl.when((i >= 1) & (i <= n))
        def _():
            c = i - 1
            s = lax.rem(c, 3)
            n_copy(c).wait_recv()
            keep_peer(c).start()
            @pl.when(stage < 3)
            def _():
                both = jnp.concatenate([n_own[lax.rem(c, 4)], n_peer[lax.rem(c, 4)]], 0)
                for j in range(hid // COLS):
                    part = pl.ds(j * COLS, COLS)
                    gate_pre, in_pre, gate_sig, gate_act = swiglu_parts(both, w_gate[:, part], w_in[:, part])
                    branch = jnp.dot((gate_act * in_pre).astype(jnp.bfloat16), w_out[part, :], preferred_element_type=jnp.float32)
                    acc[...] = branch if j == 0 else acc[...] + branch
                keep[s] = acc[:rows]
                give[s] = acc[rows:]

            keep_peer(c).wait()

            @pl.when(stage < 3)
            def _():
                give_copy(c).start()

        @pl.when(i >= 2)
        def _():
            c = i - 2
            s = lax.rem(c, 3)
            keep_h(c).wait()

            @pl.when(stage < 3)
            def _():
                give_copy(c).wait_recv()
                give_copy(c).wait_send()

                @pl.when(c >= 2)
                def _():
                    h_copy(c - 2).wait_send()

                h_out[lax.rem(c, 2)] = h_buf[lax.rem(c, DEPTH)] + (keep[s] + got[s]).astype(jnp.bfloat16)

                @pl.when(c >= DEPTH)
                def _():
                    pl.semaphore_wait(free, 1)

                h_copy(c).start()

            @pl.when((stage > 0) & (c < n - DEPTH))
            def _():
                pl.semaphore_signal(free, inc=1, device_id=before, device_id_type=pl.DeviceIdType.MESH)

        return carry

    lax.fori_loop(0, n + 2, body, 0)
    for c in range(n - 4, n):
        n_copy(c).wait_send()
        keep_own(c).wait()

    @pl.when((stage == 1) & (core == 1))
    def _():
        @pl.loop(0, n)
        def _(c):
            far_copy(c).wait_send()

    for number in range(3):
        @pl.when(hop_from[number])
        def _(number=number):
            for k in range(3):
                hop(k, number).wait_send()

    @pl.when(stage == 3)
    def _():
        keep_flipped.wait()

    for k in range(3):
        keep_weight(k).wait()

        @pl.when(home)
        def _():
            partner_block(k).wait_send()

        @pl.when(jnp.logical_not(home))
        def _():
            shared_block(k).wait_send()

            @pl.when(stage == 1)
            def _():
                away_block(k, direct).wait_send()

            @pl.when(stage != 1)
            def _():
                away_block(k, hid).wait_send()

    @pl.when(stage < 3)
    def _():
        for c in range(n - 2, n):
            h_copy(c).wait_send()


def backward_kernel(g_ref, saved_h, saved_n, *refs):
    kept = refs[:3]
    kept_t = refs[3]
    dx_ref, saved_e, saved_u, saved_da, saved_db, g_land, n_t = refs[4:11]
    (w_gate, w_in, w_out, e_buf, e_peer, n_buf, h_buf, acc, keep, give, got, e_out, u_out, da_out, db_out,
     w_sem, load_sem, n_sem, h_sem, s_send, s_recv, e_send, e_recv, g_send, g_recv, save_own, save_peer, save_u, save_da, save_db, dx_sem, dx_send, dx_recv, far_send, far_recv, raw_w, raw_n, turned, flip_sem, turn_sem, free) = refs[11:]
    n = g_ref.shape[0]
    rows = g_ref.shape[1]
    hid = w_gate.shape[1]
    stage, core, peer, after, before = stage_place()
    loads = [pltpu.make_async_copy(kept[k], (w_gate, w_in)[k], w_sem.at[k]) for k in range(2)]
    load_out = pltpu.make_async_copy(kept_t, w_out, w_sem.at[2])
    for load in loads:
        load.start()

    def cols(k):
        return pl.ds(pl.multiple_of(k * COLS, COLS), COLS)

    def flip_weight():
        def raw_load(k):
            return pltpu.make_async_copy(kept[2].at[cols(k)], raw_w.at[lax.rem(k, 2)], flip_sem.at[lax.rem(k, 2)])

        raw_load(0).start()

        @pl.loop(0, hid // COLS)
        def _(k):
            raw_load(k).wait()

            @pl.when(k + 1 < hid // COLS)
            def _():
                raw_load(k + 1).start()

            w_out[:, cols(k)] = raw_w[lax.rem(k, 2)].T

    def flip_normed():
        each = COLS // (2 * rows)
        steps = n // each

        def raw_load(k):
            return pltpu.make_async_copy(saved_n.at[pl.ds(k * each, each)], raw_n.at[lax.rem(k, 2)], flip_sem.at[lax.rem(k, 2)])

        def store(k):
            return pltpu.make_async_copy(turned.at[lax.rem(k, 2)], n_t.at[:, cols(k)], turn_sem.at[lax.rem(k, 2)])

        raw_load(0).start()

        @pl.loop(0, steps)
        def _(k):
            raw_load(k).wait()

            @pl.when(k + 1 < steps)
            def _():
                raw_load(k + 1).start()

            @pl.when(k >= 2)
            def _():
                store(k - 2).wait()

            turned[lax.rem(k, 2)] = raw_n[lax.rem(k, 2)].reshape(COLS, raw_n.shape[-1]).T
            store(k).start()

        for k in range(steps - 2, steps):
            store(k).wait()

    def g_load(c, source):
        return pltpu.make_async_copy(source.at[c], e_buf.at[lax.rem(c, DEPTH)], load_sem.at[lax.rem(c, 2)])

    def far_copy(c):
        return remote(g_ref.at[c], g_land.at[c], far_send.at[c], far_recv.at[c], {'dp': 1})

    def start_load(c):
        @pl.when(core == 1)
        def _():
            g_load(c, g_ref).start()

        @pl.when(core == 0)
        def _():
            far_copy(c).wait_recv()
            g_load(c, g_land).start()

    @pl.when((stage == 2) & (core == 0))
    def _():
        @pl.loop(0, n)
        def _(c):
            far_copy(c).start()

    def n_load(c):
        s = lax.rem(c, 3)
        return pltpu.make_async_copy(saved_n.at[c], n_buf.at[s], n_sem.at[s])

    def h_load(c):
        s = lax.rem(c, 3)
        return pltpu.make_async_copy(saved_h.at[c], h_buf.at[s], h_sem.at[s])

    def stage_copy(c):
        return remote(e_out.at[lax.rem(c, 2)], e_buf.at[lax.rem(c, DEPTH)], s_send.at[lax.rem(c, 2)], s_recv.at[lax.rem(c, DEPTH)], before)

    def e_copy(c):
        s = lax.rem(c, 3)
        return remote(e_buf.at[lax.rem(c, DEPTH)], e_peer.at[s], e_send.at[s], e_recv.at[s], peer)

    def give_copy(c):
        s = lax.rem(c, 3)
        return remote(give.at[s], got.at[s], g_send.at[s], g_recv.at[s], peer)

    def keep_own(c):
        return pltpu.make_async_copy(e_buf.at[lax.rem(c, DEPTH)], saved_e.at[c, pl.ds(0, rows)], save_own.at[lax.rem(c, 3)])

    def keep_peer(c):
        s = lax.rem(c, 3)
        return pltpu.make_async_copy(e_peer.at[s], saved_e.at[c, pl.ds(rows, rows)], save_peer.at[s])

    def keep_wide(c):
        s = lax.rem(c, 2)
        return [pltpu.make_async_copy(source.at[s], target.at[c], sem.at[s])
                for source, target, sem in ((u_out, saved_u, save_u), (da_out, saved_da, save_da), (db_out, saved_db, save_db))]

    def keep_dx(c):
        s = lax.rem(c, 2)
        return pltpu.make_async_copy(e_out.at[s], dx_ref.at[c], dx_sem.at[s])

    def dx_copy(c, k):
        s = lax.rem(c, 2)
        return remote(e_out.at[s], dx_ref.at[c], dx_send.at[s, k], dx_recv.at[0], {'dp': core, 'x': k // 2, 'core': k % 2})

    def dx_start(c):
        @pl.when(core == 0)
        def _():
            keep_dx(c).start()

        @pl.when(core == 1)
        def _():
            dx_copy(c, 0).start()

        for k in range(1, 4):
            dx_copy(c, k).start()

    def dx_done(c):
        @pl.when(core == 0)
        def _():
            keep_dx(c).wait()

        @pl.when(core == 1)
        def _():
            dx_copy(c, 0).wait_send()

        for k in range(1, 4):
            dx_copy(c, k).wait_send()

    @pl.when(stage == 3)
    def _():
        load_out.start()
        start_load(0)

    @pl.when(stage < 3)
    def _():
        flip_weight()
        flip_normed()

    def body(i, carry):
        @pl.when(i < n)
        def _():
            n_load(i).start()
            h_load(i).start()

            @pl.when(stage == 3)
            def _():
                g_load(i, g_ref).wait()

                @pl.when(i + 1 < n)
                def _():
                    start_load(i + 1)

            @pl.when(stage < 3)
            def _():
                stage_copy(i).wait_recv()

            e_copy(i).start()
            keep_own(i).start()

        @pl.when(i == 1)
        def _():
            for load in loads:
                load.wait()

            @pl.when(stage == 3)
            def _():
                load_out.wait()

        @pl.when((i >= 1) & (i <= n))
        def _():
            c = i - 1
            s = lax.rem(c, 3)
            w = lax.rem(c, 2)
            n_load(c).wait()
            e_copy(c).wait_recv()
            keep_peer(c).start()

            @pl.when(c >= 2)
            def _():
                for copy in keep_wide(c - 2):
                    copy.wait()

            normed = n_buf[s]
            both = jnp.concatenate([e_buf[lax.rem(c, DEPTH)], e_peer[s]], 0)
            for j in range(hid // COLS):
                part = pl.ds(j * COLS, COLS)
                gate_pre, in_pre, gate_sig, gate_act = swiglu_parts(normed, w_gate[:, part], w_in[:, part])
                d_hidden = jnp.dot(both, w_out[:, part], preferred_element_type=jnp.float32).astype(jnp.bfloat16).astype(jnp.float32)
                u_out[w, :, part] = (gate_act * in_pre).astype(jnp.bfloat16)
                d_gate = (d_hidden * in_pre * (gate_sig * (1.0 + gate_pre * (1.0 - gate_sig)))).astype(jnp.bfloat16)
                d_up = (d_hidden * gate_act).astype(jnp.bfloat16)
                da_out[w, :, part] = d_gate
                db_out[w, :, part] = d_up
            for copy in keep_wide(c):
                copy.start()
            acc[...] = lax.dot_general(da_out[w], w_gate[...], CONTRACT_COLS, preferred_element_type=jnp.float32) + lax.dot_general(db_out[w], w_in[...], CONTRACT_COLS, preferred_element_type=jnp.float32)
            keep[s] = acc[:rows]
            give[s] = acc[rows:]
            keep_peer(c).wait()
            give_copy(c).start()

        @pl.when(i >= 2)
        def _():
            c = i - 2
            s = lax.rem(c, 3)
            w = lax.rem(c, 2)
            h_load(c).wait()
            give_copy(c).wait_recv()
            give_copy(c).wait_send()
            e_copy(c).wait_send()
            keep_own(c).wait()

            @pl.when(c >= 2)
            def _():
                @pl.when(stage > 0)
                def _():
                    stage_copy(c - 2).wait_send()

                @pl.when(stage == 0)
                def _():
                    dx_done(c - 2)

            d_norm = keep[s] + got[s]
            h_f32, inv_rms, _ = rms_parts(h_buf[s])
            unit_rms = h_f32 * inv_rms
            d_h = inv_rms * (d_norm - unit_rms * jnp.mean(d_norm * unit_rms, axis=-1, keepdims=True))
            e_out[w] = (e_buf[lax.rem(c, DEPTH)].astype(jnp.float32) + d_h).astype(jnp.bfloat16)

            @pl.when(stage > 0)
            def _():
                @pl.when(c >= DEPTH)
                def _():
                    pl.semaphore_wait(free, 1)

                stage_copy(c).start()

            @pl.when(stage == 0)
            def _():
                dx_start(c)

            @pl.when((stage < 3) & (c < n - DEPTH))
            def _():
                pl.semaphore_signal(free, inc=1, device_id=after, device_id_type=pl.DeviceIdType.MESH)

        return carry

    lax.fori_loop(0, n + 2, body, 0)
    for c in range(n - 2, n):
        for copy in keep_wide(c):
            copy.wait()

        @pl.when(stage > 0)
        def _():
            stage_copy(c).wait_send()

        @pl.when(stage == 0)
        def _():
            dx_done(c)

    @pl.when(stage == 3)
    def _():
        flip_normed()

    @pl.when((stage > 0) | (core > 0))
    def _():
        remote(dx_ref, dx_ref, dx_send.at[0, 0], dx_recv.at[0], peer).wait_recv()

    @pl.when((stage == 2) & (core == 0))
    def _():
        @pl.loop(0, n)
        def _(c):
            far_copy(c).wait_send()


def common_scratch(width, hid, rows, flipped):
    return [pltpu.VMEM((width, hid), jnp.bfloat16), pltpu.VMEM((width, hid), jnp.bfloat16), pltpu.VMEM((width, hid) if flipped else (hid, width), jnp.bfloat16),
            pltpu.VMEM((DEPTH, rows, width), jnp.bfloat16)]


def partial_scratch(width, rows):
    return [pltpu.VMEM((2 * rows, width), jnp.float32)] + [pltpu.VMEM((3, rows, width), jnp.float32)] * 3 + [pltpu.VMEM((2, rows, width), jnp.bfloat16)]


def dma(*sizes):
    return [pltpu.SemaphoreType.DMA((size,)) for size in sizes]


def forward_phase(x_chunks, blocks):
    n, rows, width = x_chunks.shape
    half, hid = blocks[0].shape
    whole = [jax.ShapeDtypeStruct((width, hid), jnp.bfloat16)] * 2 + [jax.ShapeDtypeStruct((hid, width), jnp.bfloat16), jax.ShapeDtypeStruct((width, hid), jnp.bfloat16)]
    anywhere = pl.BlockSpec(memory_space=pl.ANY)
    return pl.pallas_call(
        forward_kernel,
        in_specs=[anywhere] * 4,
        out_specs=[anywhere] * 7,
        out_shape=[jax.ShapeDtypeStruct((n, rows, width), jnp.bfloat16), jax.ShapeDtypeStruct((n, 2 * rows, width), jnp.bfloat16), jax.ShapeDtypeStruct((n, rows, width), jnp.bfloat16)] + whole,
        scratch_shapes=common_scratch(width, hid, rows, False) + [pltpu.VMEM((4, rows, width), jnp.bfloat16)] * 2 + partial_scratch(width, rows)
        + dma(7, 2, 2, DEPTH, 4, 4, 3, 3, DEPTH, 4, 4, n, n)
        + [pltpu.VMEM((3, half, hid // RELAYED), jnp.bfloat16), pltpu.VMEM((width, hid), jnp.bfloat16), pltpu.SemaphoreType.DMA((4, 3)), pltpu.SemaphoreType.DMA((4, 3))] + [pltpu.SemaphoreType.REGULAR],
        cost_estimate=pl.CostEstimate(flops=12 * n * rows * width * hid, bytes_accessed=6 * width * hid, transcendentals=0),
        compiler_params=pltpu.CompilerParams(has_side_effects=True, vmem_limit_bytes=VMEM_BYTES),
        name="forward_phase",
    )(x_chunks, *blocks)


def backward_phase(g_chunks, saved_h, saved_n, blocks):
    n, rows, width = g_chunks.shape
    hid = blocks[0].shape[1]
    anywhere = pl.BlockSpec(memory_space=pl.ANY)
    wide = jax.ShapeDtypeStruct((n, 2 * rows, hid), jnp.bfloat16)
    return pl.pallas_call(
        backward_kernel,
        in_specs=[anywhere] * 7,
        out_specs=[anywhere] * 7,
        out_shape=[jax.ShapeDtypeStruct((n, rows, width), jnp.bfloat16), jax.ShapeDtypeStruct((n, 2 * rows, width), jnp.bfloat16), wide, wide, wide, jax.ShapeDtypeStruct((n, rows, width), jnp.bfloat16), jax.ShapeDtypeStruct((width, n * 2 * rows), jnp.bfloat16)],
        scratch_shapes=common_scratch(width, hid, rows, True)
        + [pltpu.VMEM((3, rows, width), jnp.bfloat16), pltpu.VMEM((3, 2 * rows, width), jnp.bfloat16), pltpu.VMEM((3, rows, width), jnp.bfloat16)]
        + partial_scratch(width, rows) + [pltpu.VMEM((2, 2 * rows, hid), jnp.bfloat16)] * 3
        + dma(3, 2, 3, 3, 2, DEPTH, 3, 3, 3, 3, 3, 3, 2, 2, 2, 2) + [pltpu.SemaphoreType.DMA((2, 4))] + dma(1, n, n)
        + [pltpu.VMEM((2, COLS, width), jnp.bfloat16), pltpu.VMEM((2, COLS // (2 * rows), 2 * rows, width), jnp.bfloat16), pltpu.VMEM((2, width, COLS), jnp.bfloat16)]
        + dma(2, 2) + [pltpu.SemaphoreType.REGULAR],
        cost_estimate=pl.CostEstimate(flops=20 * n * rows * width * hid, bytes_accessed=6 * width * hid, transcendentals=0),
        compiler_params=pltpu.CompilerParams(has_side_effects=True, vmem_limit_bytes=VMEM_BYTES),
        name="backward_phase",
    )(g_chunks, saved_h, saved_n, *blocks)


def gradient_kernel(n_ref, e_ref, da_ref, db_ref, u_ref, dw_gate, dw_in, dw_out,
                    raw, flipped, tile, mine, give, got, total, total_t,
                    raw_sem, tile_sem, p_send, p_recv, keep_sem, keep_t_sem, far_send, far_t_send, far_recv):
    z, y, x, core = (lax.axis_index(name) for name in ALL_AXES)
    tokens, width = e_ref.shape
    hid = da_ref.shape[1]
    half = width // 2
    tiles = hid // COLS
    steps = tokens // COLS
    home = core == y
    swap = {'dp': 1 - y, 'core': 1 - core}
    sources = (da_ref, db_ref, u_ref)
    targets = (dw_gate, dw_in, dw_out)

    def cols(j):
        return pl.ds(pl.multiple_of(j * COLS, COLS), COLS)

    def raw_load(source, k):
        return pltpu.make_async_copy(source.at[cols(k)], raw.at[lax.rem(k, 2)], raw_sem.at[lax.rem(k, 2)])

    def tile_load(a, j):
        s = lax.rem(a * tiles + j, 2)
        return pltpu.make_async_copy(sources[a].at[:, cols(j)], tile.at[s], tile_sem.at[s])

    def part_copy(t):
        s = lax.rem(t, 2)
        return remote(give.at[s], got.at[s], p_send.at[s], p_recv.at[s], {'core': 1 - core})

    def place(a, j):
        return (total_t if a == 2 else total).at[lax.rem(j, 3)], (targets[a].at[cols(j)] if a == 2 else targets[a].at[:, cols(j)])

    def home_copy(a, j):
        source, target = place(a, j)
        return pltpu.make_async_copy(source, target, (keep_t_sem if a == 2 else keep_sem).at[lax.rem(j, 3)])

    def far_copy(a, j):
        source, target = place(a, j)
        return remote(source, target, (far_t_send if a == 2 else far_send).at[lax.rem(j, 3)], far_recv.at[a], swap)

    def shipped(a, j):
        @pl.when(home)
        def _():
            home_copy(a, j).wait()

        @pl.when(jnp.logical_not(home))
        def _():
            far_copy(a, j).wait_send()

    def flip(source):
        raw_load(source, 0).start()

        @pl.loop(0, steps)
        def _(k):
            raw_load(source, k).wait()

            @pl.when(k + 1 < steps)
            def _():
                raw_load(source, k + 1).start()

            flipped[:, cols(k)] = raw[lax.rem(k, 2)].T

    whole_load = pltpu.make_async_copy(n_ref, flipped, raw_sem.at[0])
    whole_load.start()
    tile_load(0, 0).start()
    whole_load.wait()
    for a in range(3):
        if a == 2:
            flip(e_ref)

        @pl.loop(0, tiles)
        def _(j, a=a):
            t = a * tiles + j
            s = lax.rem(t, 2)
            tile_load(a, j).wait()

            @pl.when(j + 1 < tiles)
            def _():
                tile_load(a, j + 1).start()

            if a < 2:
                @pl.when(j + 1 == tiles)
                def _():
                    tile_load(a + 1, 0).start()

            @pl.when(t >= 2)
            def _():
                part_copy(t - 2).wait_send()

            @pl.loop(0, half // ROW_BLOCK)
            def _(m):
                part = pl.ds(pl.multiple_of(m * ROW_BLOCK, ROW_BLOCK), ROW_BLOCK)
                theirs = pl.ds(pl.multiple_of((1 - core) * half + m * ROW_BLOCK, ROW_BLOCK), ROW_BLOCK)
                give[s, part] = jnp.dot(flipped[theirs, :], tile[s], preferred_element_type=jnp.float32)

            part_copy(t).start()

            @pl.loop(0, half // ROW_BLOCK)
            def _(m):
                part = pl.ds(pl.multiple_of(m * ROW_BLOCK, ROW_BLOCK), ROW_BLOCK)
                ours = pl.ds(pl.multiple_of(core * half + m * ROW_BLOCK, ROW_BLOCK), ROW_BLOCK)
                mine[part] = jnp.dot(flipped[ours, :], tile[s], preferred_element_type=jnp.float32)

            @pl.when(j >= 3)
            def _():
                shipped(a, j - 3)

            if a == 1:
                @pl.when(j < 3)
                def _():
                    shipped(0, tiles - 3 + j)

            part_copy(t).wait_recv()
            w = lax.rem(j, 3)
            if a == 2:
                total_t[w] = (mine[...] + got[s]).T
            else:
                total[w] = mine[...] + got[s]

            @pl.when(home)
            def _():
                home_copy(a, j).start()

            @pl.when(jnp.logical_not(home))
            def _():
                far_copy(a, j).start()

    for a in (1, 2):
        for j in range(tiles - 3, tiles):
            shipped(a, j)
    for t in range(3 * tiles - 2, 3 * tiles):
        part_copy(t).wait_send()

    @pl.when(jnp.logical_not(home))
    def _():
        for a in range(3):
            remote(targets[a], targets[a], far_send.at[0], far_recv.at[a], swap).wait_recv()


def gradients(n_flat, e_flat, da_flat, db_flat, u_flat):
    tokens, width = e_flat.shape
    hid = da_flat.shape[1]
    half = width // 2
    anywhere = pl.BlockSpec(memory_space=pl.ANY)
    return pl.pallas_call(
        gradient_kernel,
        in_specs=[anywhere] * 5,
        out_specs=[anywhere] * 3,
        out_shape=[jax.ShapeDtypeStruct((half, hid), jnp.float32)] * 2 + [jax.ShapeDtypeStruct((hid, half), jnp.float32)],
        scratch_shapes=[pltpu.VMEM((2, COLS, width), jnp.bfloat16), pltpu.VMEM((width, tokens), jnp.bfloat16), pltpu.VMEM((2, tokens, COLS), jnp.bfloat16),
                        pltpu.VMEM((half, COLS), jnp.float32), pltpu.VMEM((2, half, COLS), jnp.float32), pltpu.VMEM((2, half, COLS), jnp.float32),
                        pltpu.VMEM((3, half, COLS), jnp.float32), pltpu.VMEM((3, COLS, half), jnp.float32)]
        + dma(2, 2, 2, 2, 3, 3, 3, 3, 3),
        cost_estimate=pl.CostEstimate(flops=6 * tokens * width * hid, bytes_accessed=6 * tokens * hid, transcendentals=0),
        compiler_params=pltpu.CompilerParams(has_side_effects=True, vmem_limit_bytes=VMEM_BYTES),
        name="gradients",
    )(n_flat, e_flat, da_flat, db_flat, u_flat)


def solution(mesh):
    fine = Mesh(mesh.devices.reshape(2, 2, 2, 2), ALL_AXES)
    act_spec = P(None, 'dp', 'tp', None)
    up_spec = P(('x', 'core'), None, 'dp', 'tp')
    down_spec = P(('x', 'core'), None, 'tp', 'dp')

    def train_step(x_in, g_out, w_gate, w_in, w_out):
        width = x_in.shape[3]
        x_in_chunks = x_in.reshape(-1, ROWS, width)
        g_in_chunks = g_out.reshape(-1, ROWS, width)
        n_chunks = x_in_chunks.shape[0]

        saved_h, saved_n, _, *weights = forward_phase(x_in_chunks, [w[0, 0] for w in (w_gate, w_in, w_out)])
        dx, saved_e, saved_u, saved_da, saved_db, _, n_t = backward_phase(g_in_chunks, saved_h, saved_n, weights)

        def flat(array):
            return array.reshape(n_chunks * 2 * ROWS, array.shape[-1])

        grads = gradients(n_t, flat(saved_e), flat(saved_da), flat(saved_db), flat(saved_u))
        dw_gate, dw_in, dw_out = (grad[None, None] for grad in grads)
        return dx.reshape(x_in.shape), dw_gate, dw_in, dw_out

    return jax.shard_map(train_step, mesh=fine, in_specs=(act_spec, act_spec, up_spec, up_spec, down_spec), out_specs=(act_spec, up_spec, up_spec, down_spec), check_vma=False)
```
